256 devices in a mesh: dp: 16 (over x_lo, z), fsdp: 16 (over y, x_hi, core).
Axes of the slice: x: 4 (x_hi: 2, x_lo: 2; x = x_hi * 2 + x_lo), y: 4, z: 8, core: 2. Of those that a mesh axis runs over, the one named last changes fastest.
Arguments:
- hidden_states: bfloat16 [32768, 8192], P(('dp', 'fsdp')), may hold values from -450 to 450
- gain: float32 [8192], replicated, may hold values from 0.1 to 1.9
- key_weight: bfloat16 [8192, 512], P('fsdp'), may hold values from -0.0625 to 0.0625
- key_cotangent: bfloat16 [32768, 512], P(('dp', 'fsdp')), may hold values from -18 to 18
- bucket: int32 [5, 32768], P(None, 'fsdp'), may hold values from 0 to 255
- sign_bits: int32 [5, 32768], P(None, 'fsdp'), may hold values from 0 to 1
- momentum: float32 [16, 5, 32768], P('fsdp', None, 'dp'), may hold values from -12 to 12
- error: float32 [16, 5, 32768], P('fsdp', None, 'dp'), may hold values from -12 to 12
Outputs:
- hidden_grad: bfloat16 [32768, 8192], P(('dp', 'fsdp'))
- momentum_new: float32 [16, 5, 32768], P('fsdp', None, 'dp')
- error_new: float32 [16, 5, 32768], P('fsdp', None, 'dp')
- update: float32 [8192, 512], P('fsdp')
The draws below stay inside these ranges and needn't reach their ends.
All inputs are finite; a program needn't handle non-finite values.
Results may differ from the reference program's by a relative error of at most 0.0095.
Values may be sent and summed in bfloat16 or wider, within the bound.
A program may use at most 128 MiB of HBM per device.

```python
import math
import jax
import jax.numpy as jnp
from jax import lax

D = 8192
ROWS = 5
NBB = 256
BLOCK = 128
KEY_WIDTH = 512
GROUP = 2048
TOKENS = 32768
NBLK = 32768
BUCKETS = 32768
TABLES = 16
N_DP = 16
N_FSDP = 16


def draw_hidden_states(key, part):
    keys = jax.random.split(key, 3)
    base = jnp.clip(jax.random.normal(keys[0], (TOKENS, D), jnp.float32), -4.0, 4.0)
    row_scale = jnp.exp(jax.random.uniform(keys[1], (TOKENS, 1), jnp.float32, 0.0, math.log(10.0)))
    col_scale = jnp.exp(jax.random.uniform(keys[2], (1, D), jnp.float32, 0.0, math.log(10.0)))
    return (base * row_scale * col_scale).astype(jnp.bfloat16)


def set_ends(result, rng, low, high):
    extent = result.shape
    spot = [jax.random.randint(jax.random.fold_in(rng, axis), (), 0, extent[axis]) for axis in range(len(extent))]
    result = result.at[tuple(spot)].set(low)
    longest = extent.index(max(extent))
    spot[longest] = (spot[longest] + 1) % extent[longest]
    return result.at[tuple(spot)].set(high)


def level_of(key, extent, cuts, low, top_value):
    def one(axis_at, blocks):
        steps = jax.random.uniform(jax.random.fold_in(jax.random.fold_in(key, 6), axis_at), (blocks,), jnp.float32, low / len(cuts), top_value / len(cuts))
        return jnp.repeat(jnp.exp(steps), extent[axis_at] // blocks).reshape((-1,) + (1,) * (len(extent) - axis_at - 1))

    factor_of = one(*cuts[0])
    for cut in cuts[1:]:
        factor_of = factor_of * one(*cut)
    return factor_of


def bell_draw(own_key, extent, spread, limit, cuts=(), kind=jnp.bfloat16):
    result = jax.random.normal(own_key, extent, jnp.float32) * spread
    if len(cuts) > 0:
        result = level_of(own_key, extent, cuts, -0.22, 0.18) * result
    return jnp.clip(result, min=-limit, max=limit).astype(kind)


def setup_inputs(seed: int = 0) -> dict:
    key_list = jax.random.split(jax.random.key(seed), 9)
    return {
        "hidden_states": draw_hidden_states(jax.random.fold_in(key_list[8], 71), 0),
        "gain": jnp.clip(1.0 + 0.18 * jax.random.normal(key_list[1], (D,), jnp.float32), 0.1, 1.9),
        "key_weight": bell_draw(key_list[2], (D, KEY_WIDTH), D ** -0.5, 0.0625, ((0, 16),)),
        "key_cotangent": bell_draw(key_list[3], (TOKENS, KEY_WIDTH), 3.0, 18.0, ((0, 256),)),
        "bucket": set_ends(jax.random.randint(key_list[4], (ROWS, NBLK), 0, NBB), jax.random.fold_in(key_list[4], 1), 0, NBB - 1).astype(jnp.int32),
        "sign_bits": set_ends(jax.random.randint(key_list[5], (ROWS, NBLK), 0, 2), jax.random.fold_in(key_list[5], 1), 0, 1).astype(jnp.int32),
        "momentum": bell_draw(key_list[6], (TABLES, ROWS, BUCKETS), 2.0, 12.0, ((0, 16), (2, 16)), jnp.float32),
        "error": bell_draw(key_list[7], (TABLES, ROWS, BUCKETS), 2.0, 12.0, ((0, 16), (2, 16)), jnp.float32),
    }


EPS = 1e-05
DECAY = 0.9
THRESHOLD = 1.0

def normalize(states, gain):
    values = states.astype(jnp.float32)
    inverse_rms = lax.rsqrt(lax.optimization_barrier(jnp.mean(values * values, axis=1, keepdims=True)) + EPS)
    normed = values * inverse_rms
    return (normed, inverse_rms, (normed * gain).astype(jnp.bfloat16))

def norm_backward(input_grad, gain, normed, inverse_rms):
    scaled = input_grad.astype(jnp.float32) * gain
    mean_term = lax.optimization_barrier(jnp.mean(scaled * normed, axis=1, keepdims=True))
    return (inverse_rms * (scaled - normed * mean_term)).astype(jnp.bfloat16)

def sketch(blocks, bucket, signs):
    slab = jnp.arange(NBLK, dtype=jnp.int32) // (NBLK // N_FSDP)
    seg_ids = (slab[None, :] * NBB + bucket).astype(jnp.int32)
    tables = jnp.stack([jax.ops.segment_sum(signs[k][:, None] * blocks, seg_ids[k], num_segments=N_FSDP * NBB) for k in range(ROWS)])
    return tables.reshape(ROWS, N_FSDP, NBB * BLOCK).transpose(1, 0, 2)

def reference(hidden_states, gain, key_weight, key_cotangent, bucket, sign_bits, momentum, error):
    signs = (2 * sign_bits - 1).astype(jnp.float32)
    grad_scale = 1.0 / math.sqrt(GROUP)

    def one_group(pair):
        states, cotangent = pair
        normed, inverse_rms, inputs = normalize(states, gain)
        input_grad = jnp.dot(cotangent, key_weight.T, preferred_element_type=jnp.float32).astype(jnp.bfloat16)
        group_grad = norm_backward(input_grad, gain, normed, inverse_rms)
        weight_grad = jnp.dot(inputs.T, cotangent, preferred_element_type=jnp.float32) * grad_scale
        return (group_grad, sketch(weight_grad.reshape(NBLK, BLOCK), bucket, signs))
    grads, tables = lax.map(one_group, (hidden_states.reshape(N_DP, GROUP, D), key_cotangent.reshape(N_DP, GROUP, KEY_WIDTH)))
    mean_table = lax.optimization_barrier(jnp.sum(tables, axis=0)) / N_DP
    momentum_new = DECAY * momentum + mean_table
    error_sum = error + momentum_new
    error_blocks = error_sum.reshape(N_FSDP, ROWS, NBB, BLOCK)
    slab = jnp.arange(NBLK, dtype=jnp.int32) // (NBLK // N_FSDP)
    row_ids = jnp.arange(ROWS, dtype=jnp.int32)
    reads = error_blocks[slab[None, :], row_ids[:, None], bucket] * signs[:, :, None]
    estimate = jnp.sort(reads, axis=0)[ROWS // 2]
    update = estimate - jnp.clip(estimate, -THRESHOLD, THRESHOLD)
    error_new = error_sum - sketch(update, bucket, signs)
    return (grads.reshape(TOKENS, D), momentum_new, error_new, update.reshape(D, KEY_WIDTH))
```

```python
import functools
import math

import jax
import jax.numpy as jnp
from jax import lax
from jax.experimental import pallas as pl
from jax.experimental.pallas import tpu as pltpu
from jax.sharding import PartitionSpec as P

ROWS = 5
NBB = 256
BLOCK = 128
EPS = 1e-05
DECAY = 0.9
THRESHOLD = 1.0
N = 16
Z = 8
BF = jnp.bfloat16
F32 = jnp.float32
MESH = pl.DeviceIdType.MESH
PLAIN = (((1,), (0,)), ((), ()))
LAST = (((1,), (1,)), ((), ()))
FIRST = (((0,), (0,)), ((), ()))
DP_ORDER = [(1, d) for d in (4, 3, 5, 2, 6, 1, 7)] + [(0, d) for d in (4, 3, 5, 2, 6, 1, 7)] + [(1, 0)]


def dot(a, b, numbers):
    return lax.dot_general(a, b, numbers, preferred_element_type=F32)


def middle_three(first, second, third):
    return jnp.maximum(jnp.minimum(first, second), jnp.minimum(jnp.maximum(first, second), third))


def middle_five(items):
    upper_pair = jnp.minimum(jnp.maximum(items[0], items[1]), jnp.maximum(items[2], items[3]))
    lower_pair = jnp.maximum(jnp.minimum(items[0], items[1]), jnp.minimum(items[2], items[3]))
    return middle_three(items[4], upper_pair, lower_pair)


def split(values):
    upper = values.astype(BF)
    return upper, (values - upper.astype(F32)).astype(BF)


def kernel(
    scale,
    hs_hbm, gain_ref, kw_hbm, cot_hbm, bucket_ref, bits_ref, mom_ref, err_ref,
    grad_hbm, mom_out, err_out, upd_out,
    hs_v, hs_rx, cot_v, cot_rx, kw_v, ig_tx, ig_rx, acc, blk, blk2, sel, table, table_bf, rs_rx, e_all,
    e_mid, out_v, gcol, inv_v, ublk, ublk2,
    load_sem, out_sem, cot_tx_s, cot_fw_s, cot_s, hs_tx_s, hs_s, ig_tx_s, ig_s, rs_tx_s, rs_s, ag_tx_s, ag_s, misc_s,
):
    dp = lax.axis_index("dp")
    me = lax.axis_index("fsdp")
    xlo, z = dp // Z, dp % Z
    y, xhi, core = me // 4, (me // 2) % 2, me % 2
    tokens, width = hs_v.shape[1], hs_v.shape[2]

    def group_slot(dy, dx, dc):
        return ((y + dy) % 4) * 4 + ((xhi + dx) % 2) * 2 + (core + dc) % 2

    def group_peer(dy, dx, dc):
        return ((xlo + dx) % 2) * Z + z, group_slot(dy, dx, dc)

    def dp_peer(dx, dz):
        return ((xlo + dx) % 2) * Z + (z + dz) % Z

    offsets = [(i // 4, (i // 2) % 2, i % 2) for i in range(1, N)]

    hs_loads = [
        pltpu.make_async_copy(hs_hbm.at[:, pl.ds(s * width, width)], hs_v.at[s], load_sem.at[s]) for s in range(N)
    ]
    cot_load = pltpu.make_async_copy(cot_hbm, cot_v, misc_s.at[0])
    kw_load = pltpu.make_async_copy(kw_hbm, kw_v, misc_s.at[1])
    for copy in hs_loads:
        copy.start()
    cot_load.start()
    kw_load.start()

    barrier = pltpu.get_barrier_semaphore()
    for off in offsets:
        pl.semaphore_signal(barrier, inc=1, device_id=group_peer(*off), device_id_type=MESH)
    for off in DP_ORDER:
        pl.semaphore_signal(barrier, inc=1, device_id=(dp_peer(*off), me), device_id_type=MESH)

    squares = jnp.zeros((tokens, BLOCK), F32)
    for s in range(N):
        hs_loads[s].wait()
        part = hs_v[s].astype(F32)
        part = part * part
        for q in range(width // BLOCK):
            squares = squares + part[:, q * BLOCK:(q + 1) * BLOCK]
    inverse = lax.rsqrt(jnp.sum(squares, axis=1, keepdims=True) / (N * width) + EPS)
    inv_v[...] = jnp.broadcast_to(inverse, (tokens, BLOCK))
    cot_load.wait()
    cot_rx[me] = (cot_v[...].astype(F32) * inverse).astype(BF)

    pl.semaphore_wait(barrier, 2 * (N - 1))

    def cot_copy(off, sem):
        return pltpu.make_async_remote_copy(
            src_ref=cot_rx.at[me], dst_ref=cot_rx.at[me], send_sem=sem, recv_sem=cot_s.at[me],
            device_id=group_peer(*off), device_id_type=MESH)

    cot_sends = [
        cot_copy(off, cot_tx_s.at[k]) for k, off in enumerate(o for o in offsets if o[2] == 0 or o == (0, 0, 1))
    ]
    for copy in cot_sends:
        copy.start()

    def hs_copy(k, off):
        return pltpu.make_async_remote_copy(
            src_ref=hs_v.at[group_slot(*off)], dst_ref=hs_rx.at[me], send_sem=hs_tx_s.at[k], recv_sem=hs_s.at[me],
            device_id=group_peer(*off), device_id_type=MESH)

    hs_sends = [hs_copy(k, off) for k, off in enumerate(offsets)]
    for copy in hs_sends:
        copy.start()
    own = pltpu.make_async_copy(hs_v.at[me], hs_rx.at[me], misc_s.at[2])
    own.start()

    gain_row = gain_ref[:, pl.ds(pl.multiple_of(me * width, width), width)]
    gcol[...] = jnp.transpose(jnp.broadcast_to(gain_row * scale, (BLOCK, width)))

    for j in range(ROWS):
        ids = jnp.broadcast_to(bucket_ref[j:j + 1, :], (16, bucket_ref.shape[1]))
        signs = jnp.broadcast_to((2 * bits_ref[j:j + 1, :] - 1).astype(F32), (16, bucket_ref.shape[1]))
        row = lax.broadcasted_iota(jnp.int32, (16, bucket_ref.shape[1]), 0)

        def fill(i, carry, j=j, ids=ids, signs=signs, row=row):
            start = pl.multiple_of(i * 16, 16)
            sel[j, pl.ds(start, 16), :] = jnp.where(ids == row + i * 16, signs, 0.0).astype(BF)
            return carry

        lax.fori_loop(0, NBB // 16, fill, 0)
    acc[...] = jnp.zeros_like(acc)
    kw_load.wait()
    own.wait()

    def wait_slot(buffer, sem, slot):
        pltpu.make_async_remote_copy(
            src_ref=buffer.at[slot], dst_ref=buffer.at[slot], send_sem=misc_s.at[3], recv_sem=sem.at[slot],
            device_id=group_peer(0, 0, 1), device_id_type=MESH).wait_recv()

    def forward(i):
        slot = group_slot(4 - i // 2, i % 2, 0)
        return slot, pltpu.make_async_remote_copy(
            src_ref=cot_rx.at[slot], dst_ref=cot_rx.at[slot], send_sem=cot_fw_s.at[i], recv_sem=cot_s.at[slot],
            device_id=group_peer(0, 0, 1), device_id_type=MESH)

    for i in range(1, N // 2):
        slot, copy = forward(i)
        wait_slot(cot_rx, cot_s, slot)
        copy.start()

    def input_grad(i, carry):
        chip = ((y + 4 - i // 2) % 4) * 2 + (xhi + i) % 2
        other = chip * 2 + (core + 1) % 2
        wait_slot(cot_rx, cot_s, other)
        rows = cot_rx[pl.ds(chip * 2, 2)].reshape(2 * tokens, cot_rx.shape[2])
        product = dot(rows, kw_v[...], LAST).astype(BF)
        ig_tx[pl.ds(chip * 2, 2)] = product.reshape(2, tokens, width)
        return carry

    lax.fori_loop(0, N // 2, input_grad, 0)

    def accumulate(chip):
        rows = hs_rx[pl.ds(chip * 2, 2)].reshape(2 * tokens, width)
        cots = cot_rx[pl.ds(chip * 2, 2)].reshape(2 * tokens, cot_rx.shape[2])
        acc[...] += dot(rows, cots, FIRST)

    def chip_of(i):
        return ((y + 4 - i // 2) % 4) * 2 + (xhi + i) % 2

    def weight_grad(i, carry):
        chip = chip_of(i)
        wait_slot(hs_rx, hs_s, chip * 2 + (core + 1) % 2)

        @pl.when(i > 0)
        def _():
            wait_slot(hs_rx, hs_s, chip * 2 + core)

        accumulate(chip)
        return carry

    lax.fori_loop(0, N // 2, weight_grad, 0)

    ig_sends = [
        pltpu.make_async_remote_copy(
            src_ref=ig_tx.at[group_slot(*off)], dst_ref=ig_rx.at[me], send_sem=ig_tx_s.at[k], recv_sem=ig_s.at[me],
            device_id=group_peer(*off), device_id_type=MESH)
        for k, off in enumerate(offsets)
    ]
    for copy in ig_sends:
        copy.start()
    ig_own = pltpu.make_async_copy(ig_tx.at[me], ig_rx.at[me], misc_s.at[4])
    ig_own.start()

    parts = width // BLOCK
    for q in range(parts):
        blk[pl.ds(q, width, stride=parts), :] = acc[:, q * BLOCK:(q + 1) * BLOCK] * gcol[...]

    def to_halves(i, carry):
        rows = pl.ds(pl.multiple_of(i * 256, 256), 256)
        upper, lower = split(blk[rows, :])
        blk2[rows, 0:BLOCK] = upper
        blk2[rows, BLOCK:] = lower
        return carry

    lax.fori_loop(0, blk.shape[0] // 256, to_halves, 0)

    def sketch_row(j, carry):
        both = dot(sel[j], blk2[...], PLAIN)
        total = both[:, :BLOCK] + both[:, BLOCK:]
        table[j] = total
        table_bf[j] = total.astype(BF)
        return carry

    lax.fori_loop(0, ROWS, sketch_row, 0)

    share = NBB // N
    rs_sends = []
    for k, off in enumerate(DP_ORDER):
        target = dp_peer(*off)
        rs_sends.append(pltpu.make_async_remote_copy(
            src_ref=table_bf.at[:, pl.ds(pl.multiple_of(target * share, share), share), :], dst_ref=rs_rx.at[dp],
            send_sem=rs_tx_s.at[k], recv_sem=rs_s.at[dp], device_id=(target, me), device_id_type=MESH))
    for copy in rs_sends:
        copy.start()
    mine = pl.ds(pl.multiple_of(dp * share, share), share)
    for t in range(share):
        e_mid[0, :, t, :] = mom_ref[0, :, t * BLOCK:(t + 1) * BLOCK]
        e_mid[1, :, t, :] = err_ref[0, :, t * BLOCK:(t + 1) * BLOCK]
    total = table[:, mine, :]
    for off in DP_ORDER:
        source = dp_peer(*off)
        pltpu.make_async_remote_copy(
            src_ref=rs_rx.at[source], dst_ref=rs_rx.at[source], send_sem=misc_s.at[3], recv_sem=rs_s.at[source],
            device_id=(source, me), device_id_type=MESH).wait_recv()
        total = total + rs_rx[source].astype(F32)
    momentum_new = DECAY * e_mid[0] + total
    error_sum = e_mid[1] + momentum_new
    e_mid[0] = momentum_new
    e_mid[1] = error_sum
    e_all[:, mine, :] = error_sum.astype(BF)
    for t in range(share):
        mom_out[0, :, t * BLOCK:(t + 1) * BLOCK] = e_mid[0, :, t, :]
    ag_sends = []
    for k, off in enumerate(DP_ORDER):
        ag_sends.append(pltpu.make_async_remote_copy(
            src_ref=e_all.at[:, mine, :], dst_ref=e_all.at[:, mine, :], send_sem=ag_tx_s.at[k],
            recv_sem=ag_s.at[dp], device_id=(dp_peer(*off), me), device_id_type=MESH))
    for copy in ag_sends:
        copy.start()

    ig_own.wait()

    def row_sums(i, carry):
        chip = chip_of(i)
        wait_slot(ig_rx, ig_s, chip * 2 + (core + 1) % 2)

        @pl.when(i > 0)
        def _():
            wait_slot(ig_rx, ig_s, chip * 2 + core)

        for h in range(2):
            slot = chip * 2 + h
            gains = gain_ref[:, pl.ds(pl.multiple_of(slot * width, width), width)]
            product = ig_rx[slot].astype(F32) * hs_v[slot].astype(F32) * gains
            for q in range(parts):
                carry = carry + product[:, q * BLOCK:(q + 1) * BLOCK]
        return carry

    sums = lax.fori_loop(0, N // 2, row_sums, jnp.zeros((tokens, BLOCK), F32))
    mean_term = jnp.sum(sums, axis=1, keepdims=True) / (N * width)
    inverse = inv_v[:, 0:1]
    factor = inverse * inverse * mean_term

    def grad_copy(s):
        return pltpu.make_async_copy(
            out_v.at[s], grad_hbm.at[:, pl.ds(pl.multiple_of(s * width, width), width)], out_sem.at[s])

    def hidden(s, carry):
        gains = gain_ref[:, pl.ds(pl.multiple_of(s * width, width), width)]
        out_v[s] = (ig_rx[s].astype(F32) * gains - hs_v[s].astype(F32) * factor).astype(BF)
        grad_copy(s).start()
        return carry

    lax.fori_loop(0, N, hidden, 0)

    for off in DP_ORDER:
        source = dp_peer(*off)
        theirs = pl.ds(pl.multiple_of(source * share, share), share)
        pltpu.make_async_remote_copy(
            src_ref=e_all.at[:, theirs, :], dst_ref=e_all.at[:, theirs, :], send_sem=misc_s.at[3],
            recv_sem=ag_s.at[source], device_id=(source, me), device_id_type=MESH).wait_recv()

    def estimate(i, carry):
        start = pl.multiple_of(i * 512, 512)
        reads = [dot(e_all[j], sel[j, :, pl.ds(start, 512)], FIRST) for j in range(ROWS)]
        middle = middle_five(reads)
        update = jnp.transpose(middle - jnp.clip(middle, -THRESHOLD, THRESHOLD))
        rows = pl.ds(start, 512)
        ublk[rows, :] = update
        upper, lower = split(update)
        ublk2[rows, 0:BLOCK] = upper
        ublk2[rows, BLOCK:] = lower
        return carry

    lax.fori_loop(0, ublk.shape[0] // 512, estimate, 0)
    for q in range(parts):
        upd_out[:, q * BLOCK:(q + 1) * BLOCK] = ublk[pl.ds(q, width, stride=parts), :]
    selected = sel[:, mine, :].reshape(ROWS * share, sel.shape[2])
    both = dot(selected, ublk2[...], PLAIN)
    e_mid[1] = e_mid[1] - (both[:, :BLOCK] + both[:, BLOCK:]).reshape(ROWS, share, BLOCK)
    for t in range(share):
        err_out[0, :, t * BLOCK:(t + 1) * BLOCK] = e_mid[1, :, t, :]

    for copy in cot_sends + hs_sends + ig_sends + rs_sends + ag_sends:
        copy.wait_send()
    for i in range(1, N // 2):
        forward(i)[1].wait_send()
    for s in range(N):
        grad_copy(s).wait()


def on_device(hidden_states, gain, key_weight, key_cotangent, bucket, sign_bits, momentum, error):
    tokens, model = hidden_states.shape
    width, keys = key_weight.shape
    count = bucket.shape[1]
    scale = 1.0 / math.sqrt(tokens * N) / N
    any_spec = pl.BlockSpec(memory_space=pl.ANY)
    vmem = pl.BlockSpec(memory_space=pltpu.VMEM)
    dma = pltpu.SemaphoreType.DMA
    share = momentum.shape[2] // BLOCK
    return pl.pallas_call(
        functools.partial(kernel, scale),
        out_shape=(
            jax.ShapeDtypeStruct((tokens, model), BF),
            jax.ShapeDtypeStruct(momentum.shape, F32),
            jax.ShapeDtypeStruct(error.shape, F32),
            jax.ShapeDtypeStruct((width, keys), F32),
        ),
        in_specs=[any_spec, vmem, any_spec, any_spec, vmem, vmem, vmem, vmem],
        out_specs=(any_spec, vmem, vmem, vmem),
        scratch_shapes=[
            pltpu.VMEM((N, tokens, width), BF),
            pltpu.VMEM((N, tokens, width), BF),
            pltpu.VMEM((tokens, keys), BF),
            pltpu.VMEM((N, tokens, keys), BF),
            pltpu.VMEM((width, keys), BF),
            pltpu.VMEM((N, tokens, width), BF),
            pltpu.VMEM((N, tokens, width), BF),
            pltpu.VMEM((width, keys), F32),
            pltpu.VMEM((count, BLOCK), F32),
            pltpu.VMEM((count, 2 * BLOCK), BF),
            pltpu.VMEM((ROWS, NBB, count), BF),
            pltpu.VMEM((ROWS, NBB, BLOCK), F32),
            pltpu.VMEM((ROWS, NBB, BLOCK), BF),
            pltpu.VMEM((N, ROWS, share, BLOCK), BF),
            pltpu.VMEM((ROWS, NBB, BLOCK), BF),
            pltpu.VMEM((2, ROWS, share, BLOCK), F32),
            pltpu.VMEM((N, tokens, width), BF),
            pltpu.VMEM((width, BLOCK), F32),
            pltpu.VMEM((tokens, BLOCK), F32),
            pltpu.VMEM((count, BLOCK), F32),
            pltpu.VMEM((count, 2 * BLOCK), BF),
            dma((N,)), dma((N,)), dma((8,)), dma((8,)), dma((N,)), dma((N,)), dma((N,)), dma((N,)), dma((N,)),
            dma((N,)), dma((N,)), dma((N,)), dma((N,)), dma((8,)),
        ],
        compiler_params=pltpu.CompilerParams(
            collective_id=0, has_side_effects=True, vmem_limit_bytes=60 * 1024 * 1024),
        name="step",
    )(hidden_states, gain.reshape(1, model), key_weight, key_cotangent, bucket, sign_bits, momentum, error)


def solution(mesh):
    in_specs = (
        P(("dp", "fsdp"), None),
        P(),
        P("fsdp", None),
        P(("dp", "fsdp"), None),
        P(None, "fsdp"),
        P(None, "fsdp"),
        P("fsdp", None, "dp"),
        P("fsdp", None, "dp"),
    )
    out_specs = (
        P(("dp", "fsdp"), None),
        P("fsdp", None, "dp"),
        P("fsdp", None, "dp"),
        P("fsdp", None),
    )
    return jax.shard_map(
        on_device, mesh=mesh, in_specs=in_specs, out_specs=out_specs, check_vma=False
    )
```

```python
import functools
import math

import jax
import jax.numpy as jnp
from jax import lax
from jax.experimental import pallas as pl
from jax.experimental.pallas import tpu as pltpu
from jax.sharding import PartitionSpec as P

ROWS = 5
NBB = 256
BLOCK = 128
EPS = 1e-05
DECAY = 0.9
THRESHOLD = 1.0
N = 16
BLK = 4
Z = 8
BF = jnp.bfloat16
F32 = jnp.float32
MESH = pl.DeviceIdType.MESH
PLAIN = (((1,), (0,)), ((), ()))
LAST = (((1,), (1,)), ((), ()))
FIRST = (((0,), (0,)), ((), ()))
DP_ORDER = [(1, d) for d in (4, 3, 5, 2, 6, 1, 7)] + [(0, d) for d in (4, 3, 5, 2, 6, 1, 7)] + [(1, 0)]


def dot(a, b, numbers):
    return lax.dot_general(a, b, numbers, preferred_element_type=F32)


def middle_three(first, second, third):
    return jnp.maximum(jnp.minimum(first, second), jnp.minimum(jnp.maximum(first, second), third))


def middle_five(items):
    upper_pair = jnp.minimum(jnp.maximum(items[0], items[1]), jnp.maximum(items[2], items[3]))
    lower_pair = jnp.maximum(jnp.minimum(items[0], items[1]), jnp.minimum(items[2], items[3]))
    return middle_three(items[4], upper_pair, lower_pair)


def split(values):
    upper = values.astype(BF)
    return upper, (values - upper.astype(F32)).astype(BF)


def kernel(
    scale,
    hs_hbm, gain_ref, kw_hbm, cot_hbm, bucket_ref, bits_ref, mom_ref, err_ref,
    grad_hbm, mom_out, err_out, upd_out,
    hs_v, hs_rx, cot_v, cot_rx, kw_v, ig_tx, ig_rx, acc, blk, blk2, sel, table_bf, rs_rx, e_all,
    e_mid, out_v, gcol, inv_v, ublk, ublk2, sel_h, bucket_h, bits_h,
    load_sem, out_sem, cot_tx_s, cot_s, hs_tx_s, hs_s, ig_tx_s, ig_s, rs_tx_s, rs_s, ag_tx_s, ag_s, misc_s,
    shared_tx_s, shared_s,
):
    dp = lax.axis_index("dp")
    me = lax.axis_index("fsdp")
    xlo, z = dp // Z, dp % Z
    y, xhi, core = me // 4, (me // 2) % 2, me % 2
    tokens, width = hs_v.shape[1], hs_v.shape[2]

    def other(value):
        return value + 1 - 2 * (value % 2)

    def pick(kind, first, second):
        return first + kind * (second - first)

    def block_chip(kind, p):
        bx, by = p // 2, p % 2
        return (
            xhi + bx * pick(kind, 1 - 2 * xhi, 0),
            xlo + bx * (1 - 2 * xlo),
            y + by * (pick(kind, other(y), 3 - y) - y),
        )

    def held_slab(hi, lo, yy, kind, j):
        held_y = pick(kind, 3 - yy, other(yy)) if j else yy
        return held_y * 4 + pick(kind, hi, 1 - lo if j else lo) * 2 + kind

    def device(hi, lo, yy, zz, kind):
        return lo * Z + zz, yy * 4 + hi * 2 + kind

    def target(dc, p):
        kind = (core + dc) % 2
        return device(*block_chip(kind, p), z, kind)

    def target_slab(dc, p, j):
        kind = (core + dc) % 2
        return held_slab(*block_chip(kind, p), kind, j)

    def source(dc, p):
        return device(*block_chip(core, p), z, (core + dc) % 2)

    def dp_peer(dx, dz):
        return ((xlo + dx) % 2) * Z + (z + dz) % Z

    held = [held_slab(xhi, xlo, y, core, j) for j in range(2)]
    own_slab = held[0] == me
    unit = [pick(core, xlo, xhi), pick(core, xlo, 1 - xhi)]
    my_index = [unit[j] * Z + z for j in range(2)]

    def holder(j, dx, dz):
        u, zz = (xlo + dx) % 2, (z + Z - dz) % Z
        yy = pick(core, 3 - y, other(y)) if j else y
        hi, lo = (1 - u, 1 - xhi) if j else (u, xhi)
        return u * Z + zz, device(pick(core, xhi, hi), pick(core, u, lo), yy, zz, core)

    def owner(j, dx, dz):
        share_index = ((unit[j] + dx) % 2) * Z + (z + dz) % Z
        return share_index, (share_index, held[j])

    partner = [owner(j, 0, 0)[1] for j in range(2)]
    offsets = [(dc, p) for p in range(BLK) for dc in range(2) if (dc, p) != (0, 0)]

    hs_loads = [
        pltpu.make_async_copy(hs_hbm.at[:, pl.ds(s * width, width)], hs_v.at[s], load_sem.at[s]) for s in range(N)
    ]
    cot_load = pltpu.make_async_copy(cot_hbm, cot_v, misc_s.at[0])
    for copy in hs_loads:
        copy.start()
    cot_load.start()

    barrier = pltpu.get_barrier_semaphore()
    ready = 0
    for dc, p in offsets:
        pl.semaphore_signal(barrier, inc=1, device_id=source(dc, p), device_id_type=MESH)
        ready += 1
        if dc == 1 and p > 0:
            pl.semaphore_signal(barrier, inc=1, device_id=target(dc, p), device_id_type=MESH)
            ready += 1
    for off in DP_ORDER:
        pl.semaphore_signal(barrier, inc=1, device_id=(dp_peer(off[0], Z - off[1]), me), device_id_type=MESH)
        for j in range(2):
            pl.semaphore_signal(barrier, inc=1, device_id=holder(j, *off)[1], device_id_type=MESH)
        ready += 3

    for j in range(2):
        pl.semaphore_signal(barrier, inc=1, device_id=partner[j], device_id_type=MESH)
        ready += 1

    squares = jnp.zeros((tokens, BLOCK), F32)
    for s in range(N):
        hs_loads[s].wait()
        part = hs_v[s].astype(F32)
        part = part * part
        for q in range(width // BLOCK):
            squares = squares + part[:, q * BLOCK:(q + 1) * BLOCK]
    inverse = lax.rsqrt(jnp.sum(squares, axis=1, keepdims=True) / (N * width) + EPS)
    inv_v[...] = jnp.broadcast_to(inverse, (tokens, BLOCK))
    cot_load.wait()
    cot_rx[core] = (cot_v[...].astype(F32) * inverse).astype(BF)

    pl.semaphore_wait(barrier, ready)

    def shared(j):
        return [(bucket_ref, bucket_h.at[j], 2 * j), (bits_ref, bits_h.at[j], 2 * j + 1), (kw_hbm, kw_v.at[j], 4 + j)]

    def to_partner(j, item):
        src, dst, k = item
        return pltpu.make_async_remote_copy(
            src_ref=src, dst_ref=dst, send_sem=shared_tx_s.at[k], recv_sem=shared_s.at[k],
            device_id=partner[j], device_id_type=MESH)

    def to_self(item):
        src, dst, k = item
        return pltpu.make_async_copy(src, dst, shared_s.at[k])

    def send_shared(pick_items):
        @pl.when(jnp.logical_not(own_slab))
        def _():
            for item in pick_items(shared(0)):
                to_partner(0, item).start()

        @pl.when(own_slab)
        def _():
            for item in pick_items(shared(0)):
                to_self(item).start()

        for item in pick_items(shared(1)):
            to_partner(1, item).start()

    send_shared(lambda items: items[:2])

    cot_sends = [
        pltpu.make_async_remote_copy(
            src_ref=cot_rx.at[core], dst_ref=cot_rx.at[2 * p + core], send_sem=cot_tx_s.at[k],
            recv_sem=cot_s.at[2 * p + core], device_id=target(dc, p), device_id_type=MESH)
        for k, (dc, p) in enumerate(offsets)
    ]
    for copy in cot_sends:
        copy.start()
    hs_sends = [
        pltpu.make_async_remote_copy(
            src_ref=hs_v.at[target_slab(dc, p, j)], dst_ref=hs_rx.at[j * 2 * BLK + 2 * p + core],
            send_sem=hs_tx_s.at[j * 2 * BLK + k],
            recv_sem=hs_s.at[j * 2 * BLK + 2 * p + core], device_id=target(dc, p), device_id_type=MESH)
        for j in range(2) for k, (dc, p) in enumerate(offsets)
    ]
    for copy in hs_sends:
        copy.start()
    own = [
        pltpu.make_async_copy(hs_v.at[held[j]], hs_rx.at[j * 2 * BLK + core], misc_s.at[1 + j]) for j in range(2)
    ]
    for copy in own:
        copy.start()
    send_shared(lambda items: items[2:])

    for j in range(2):
        gain_row = gain_ref[:, pl.ds(pl.multiple_of(held[j] * width, width), width)]
        gcol[j] = jnp.transpose(jnp.broadcast_to(gain_row * scale, (BLOCK, width)))

    def selectors(ids_ref, sign_ref, out):
        for j in range(ROWS):
            ids = jnp.broadcast_to(ids_ref[j:j + 1, :], (16, ids_ref.shape[1]))
            signs = jnp.broadcast_to((2 * sign_ref[j:j + 1, :] - 1).astype(F32), (16, ids_ref.shape[1]))
            row = lax.broadcasted_iota(jnp.int32, (16, ids_ref.shape[1]), 0)

            def fill(i, carry, j=j, ids=ids, signs=signs, row=row):
                start = pl.multiple_of(i * 16, 16)
                out[j, pl.ds(start, 16), :] = jnp.where(ids == row + i * 16, signs, 0.0).astype(BF)
                return carry

            lax.fori_loop(0, NBB // 16, fill, 0)

    acc[...] = jnp.zeros_like(acc)
    for j in range(2):
        for item in shared(j)[:2]:
            to_self(item).wait()
        selectors(bucket_h.at[j], bits_h.at[j], sel_h.at[j])
    selectors(bucket_ref, bits_ref, sel)
    for copy in own:
        copy.wait()

    def wait_slot(buffer, sem, slot):
        pltpu.make_async_remote_copy(
            src_ref=buffer.at[slot], dst_ref=buffer.at[slot], send_sem=misc_s.at[3], recv_sem=sem.at[slot],
            device_id=target(1, 0), device_id_type=MESH).wait_recv()

    parts = width // BLOCK
    share = NBB // N

    def half_weight_grad(j):
        def weight_grad(p, carry):
            if j == 0:
                wait_slot(cot_rx, cot_s, 2 * p + (core + 1) % 2)
            wait_slot(hs_rx, hs_s, j * 2 * BLK + 2 * p + (core + 1) % 2)

            @pl.when(p > 0)
            def _():
                if j == 0:
                    wait_slot(cot_rx, cot_s, 2 * p + core)
                wait_slot(hs_rx, hs_s, j * 2 * BLK + 2 * p + core)

            rows = hs_rx[pl.ds(j * 2 * BLK + p * 2, 2)].reshape(2 * tokens, width)
            cots = cot_rx[pl.ds(p * 2, 2)].reshape(2 * tokens, cot_rx.shape[2])
            acc[j] += dot(rows, cots, FIRST)
            return carry

        lax.fori_loop(0, BLK, weight_grad, 0)

        for q in range(parts):
            blk[pl.ds(q, width, stride=parts), :] = acc[j, :, q * BLOCK:(q + 1) * BLOCK] * gcol[j]

        def to_halves(i, carry):
            rows = pl.ds(pl.multiple_of(i * 256, 256), 256)
            upper, lower = split(blk[rows, :])
            blk2[rows, 0:BLOCK] = upper
            blk2[rows, BLOCK:] = lower
            return carry

        lax.fori_loop(0, blk.shape[0] // 256, to_halves, 0)

        def sketch_row(i, carry):
            both = dot(sel_h[j, i], blk2[...], PLAIN)
            table_bf[j, i] = (both[:, :BLOCK] + both[:, BLOCK:]).astype(BF)
            return carry

        lax.fori_loop(0, ROWS, sketch_row, 0)

    def share_copy(j, k, off):
        index, place = owner(j, *off)
        return pltpu.make_async_remote_copy(
            src_ref=table_bf.at[j, :, pl.ds(pl.multiple_of(index * share, share), share), :],
            dst_ref=rs_rx.at[j * N + my_index[j]], send_sem=rs_tx_s.at[j * N + k],
            recv_sem=rs_s.at[j * N + my_index[j]],
            device_id=place, device_id_type=MESH)

    def ig_copy(j, k, dc, p):
        return pltpu.make_async_remote_copy(
            src_ref=ig_tx.at[j * 2 * BLK + 2 * p + (core + dc) % 2], dst_ref=ig_rx.at[held[j]],
            send_sem=ig_tx_s.at[j * 2 * BLK + k],
            recv_sem=ig_s.at[held[j]], device_id=source(dc, p), device_id_type=MESH)

    ig_sends = [ig_copy(j, k, dc, p) for j in range(2) for k, (dc, p) in enumerate(offsets)]
    ig_own = [
        pltpu.make_async_copy(ig_tx.at[j * 2 * BLK + core], ig_rx.at[held[j]], misc_s.at[4 + j]) for j in range(2)
    ]

    def send_input_grad(j):
        to_self(shared(j)[2]).wait()

        def input_grad(p, carry):
            rows = cot_rx[pl.ds(p * 2, 2)].reshape(2 * tokens, cot_rx.shape[2])
            product = dot(rows, kw_v[j], LAST).astype(BF)
            ig_tx[pl.ds(j * 2 * BLK + p * 2, 2)] = product.reshape(2, tokens, width)
            return carry

        lax.fori_loop(0, BLK, input_grad, 0)
        for k, (dc, p) in enumerate(offsets):
            ig_copy(j, k, dc, p).start()
        pltpu.make_async_copy(ig_tx.at[j * 2 * BLK + core], ig_rx.at[held[j]], misc_s.at[4 + j]).start()

    rs_sends = []
    for j in range(2):
        half_weight_grad(j)
        sends = [share_copy(j, k, off) for k, off in enumerate(DP_ORDER)]
        for copy in sends:
            copy.start()
        rs_sends += sends
        if j == 1:
            rs_sends.append(share_copy(1, N - 1, (0, 0)))
            rs_sends[-1].start()
        else:
            @pl.when(jnp.logical_not(own_slab))
            def _():
                share_copy(0, N - 1, (0, 0)).start()

            @pl.when(own_slab)
            def _():
                pltpu.make_async_copy(
                    table_bf.at[0, :, pl.ds(pl.multiple_of(my_index[0] * share, share), share), :],
                    rs_rx.at[my_index[0]], rs_s.at[my_index[0]]).start()
                send_input_grad(0)

    for j in range(2):
        if j == 0:
            pl.when(jnp.logical_not(own_slab))(lambda: send_input_grad(0))
        else:
            send_input_grad(1)

    mine = pl.ds(pl.multiple_of(dp * share, share), share)
    total = jnp.zeros((ROWS, share, BLOCK), F32)
    for j in range(2):
        for off in DP_ORDER + [(0, 0)]:
            index = j * N + holder(j, *off)[0]
            pltpu.make_async_copy(rs_rx.at[index], rs_rx.at[index], rs_s.at[index]).wait()
            total = total + rs_rx[index].astype(F32)
    momentum_new = DECAY * mom_ref[...] + total
    error_sum = err_ref[...] + momentum_new
    mom_out[...] = momentum_new
    e_mid[...] = error_sum
    e_all[:, mine, :] = error_sum.astype(BF)
    ag_sends = []
    for k, off in enumerate(DP_ORDER):
        ag_sends.append(pltpu.make_async_remote_copy(
            src_ref=e_all.at[:, mine, :], dst_ref=e_all.at[:, mine, :], send_sem=ag_tx_s.at[k],
            recv_sem=ag_s.at[dp], device_id=(dp_peer(*off), me), device_id_type=MESH))
    for copy in ag_sends:
        copy.start()

    for off in DP_ORDER:
        index = dp_peer(*off)
        theirs = pl.ds(pl.multiple_of(index * share, share), share)
        pltpu.make_async_remote_copy(
            src_ref=e_all.at[:, theirs, :], dst_ref=e_all.at[:, theirs, :], send_sem=misc_s.at[3],
            recv_sem=ag_s.at[index], device_id=(index, me), device_id_type=MESH).wait_recv()

    def estimate(i, carry):
        start = pl.multiple_of(i * 512, 512)
        reads = [dot(e_all[j], sel[j, :, pl.ds(start, 512)], FIRST) for j in range(ROWS)]
        middle = middle_five(reads)
        update = jnp.transpose(middle - jnp.clip(middle, -THRESHOLD, THRESHOLD))
        rows = pl.ds(start, 512)
        ublk[rows, :] = update
        upper, lower = split(update)
        ublk2[rows, 0:BLOCK] = upper
        ublk2[rows, BLOCK:] = lower
        return carry

    lax.fori_loop(0, ublk.shape[0] // 512, estimate, 0)
    for q in range(parts):
        upd_out[:, q * BLOCK:(q + 1) * BLOCK] = ublk[pl.ds(q, width, stride=parts), :]
    selected = sel[:, mine, :].reshape(ROWS * share, sel.shape[2])
    both = dot(selected, ublk2[...], PLAIN)
    err_out[...] = e_mid[...] - (both[:, :BLOCK] + both[:, BLOCK:]).reshape(ROWS, share, BLOCK)

    for copy in ig_own:
        copy.wait()

    def row_sums(p, carry):
        for j in range(2):
            for dc in range(2):
                slot = target_slab(dc, p, j)
                if dc == 1:
                    wait_slot(ig_rx, ig_s, slot)
                else:
                    @pl.when(p > 0)
                    def _(slot=slot):
                        wait_slot(ig_rx, ig_s, slot)

                gains = gain_ref[:, pl.ds(pl.multiple_of(slot * width, width), width)]
                product = ig_rx[slot].astype(F32) * hs_v[slot].astype(F32) * gains
                for q in range(parts):
                    carry = carry + product[:, q * BLOCK:(q + 1) * BLOCK]
        return carry

    sums = lax.fori_loop(0, BLK, row_sums, jnp.zeros((tokens, BLOCK), F32))
    mean_term = jnp.sum(sums, axis=1, keepdims=True) / (N * width)
    inverse = inv_v[:, 0:1]
    factor = inverse * inverse * mean_term

    def grad_copy(s):
        return pltpu.make_async_copy(
            out_v.at[s], grad_hbm.at[:, pl.ds(pl.multiple_of(s * width, width), width)], out_sem.at[s])

    def hidden(s, carry):
        gains = gain_ref[:, pl.ds(pl.multiple_of(s * width, width), width)]
        out_v[s] = (ig_rx[s].astype(F32) * gains - hs_v[s].astype(F32) * factor).astype(BF)
        grad_copy(s).start()
        return carry

    lax.fori_loop(0, N, hidden, 0)

    for copy in cot_sends + hs_sends + ig_sends + rs_sends + ag_sends:
        copy.wait_send()

    for item in shared(1):
        to_partner(1, item).wait_send()

    @pl.when(jnp.logical_not(own_slab))
    def _():
        for item in shared(0):
            to_partner(0, item).wait_send()
        share_copy(0, N - 1, (0, 0)).wait_send()

    for s in range(N):
        grad_copy(s).wait()


def on_device(hidden_states, gain, key_weight, key_cotangent, bucket, sign_bits, momentum, error):
    tokens, model = hidden_states.shape
    width, keys = key_weight.shape
    count = bucket.shape[1]
    scale = 1.0 / math.sqrt(tokens * N) / N
    any_spec = pl.BlockSpec(memory_space=pl.ANY)
    vmem = pl.BlockSpec(memory_space=pltpu.VMEM)
    dma = pltpu.SemaphoreType.DMA
    share = momentum.shape[2] // BLOCK
    flat = (ROWS, share, BLOCK)
    grad, momentum_new, error_new, update = pl.pallas_call(
        functools.partial(kernel, scale),
        out_shape=(
            jax.ShapeDtypeStruct((tokens, model), BF),
            jax.ShapeDtypeStruct((ROWS, share, BLOCK), F32),
            jax.ShapeDtypeStruct((ROWS, share, BLOCK), F32),
            jax.ShapeDtypeStruct((width, keys), F32),
        ),
        in_specs=[any_spec, vmem, any_spec, any_spec, vmem, vmem, vmem, vmem],
        out_specs=(any_spec, vmem, vmem, vmem),
        scratch_shapes=[
            pltpu.VMEM((N, tokens, width), BF),
            pltpu.VMEM((N, tokens, width), BF),
            pltpu.VMEM((tokens, keys), BF),
            pltpu.VMEM((2 * BLK, tokens, keys), BF),
            pltpu.VMEM((2, width, keys), BF),
            pltpu.VMEM((N, tokens, width), BF),
            pltpu.VMEM((N, tokens, width), BF),
            pltpu.VMEM((2, width, keys), F32),
            pltpu.VMEM((count, BLOCK), F32),
            pltpu.VMEM((count, 2 * BLOCK), BF),
            pltpu.VMEM((ROWS, NBB, count), BF),
            pltpu.VMEM((2, ROWS, NBB, BLOCK), BF),
            pltpu.VMEM((2 * N, ROWS, share, BLOCK), BF),
            pltpu.VMEM((ROWS, NBB, BLOCK), BF),
            pltpu.VMEM((ROWS, share, BLOCK), F32),
            pltpu.VMEM((N, tokens, width), BF),
            pltpu.VMEM((2, width, BLOCK), F32),
            pltpu.VMEM((tokens, BLOCK), F32),
            pltpu.VMEM((count, BLOCK), F32),
            pltpu.VMEM((count, 2 * BLOCK), BF),
            pltpu.VMEM((2, ROWS, NBB, count), BF),
            pltpu.VMEM((2,) + bucket.shape, jnp.int32),
            pltpu.VMEM((2,) + bucket.shape, jnp.int32),
            dma((N,)), dma((N,)), dma((8,)), dma((8,)), dma((N,)), dma((N,)), dma((N,)), dma((N,)),
            dma((2 * N,)), dma((2 * N,)), dma((N,)), dma((N,)), dma((8,)), dma((8,)), dma((8,)),
        ],
        compiler_params=pltpu.CompilerParams(
            collective_id=0, has_side_effects=True, vmem_limit_bytes=60 * 1024 * 1024),
        name="step",
    )(hidden_states, gain.reshape(1, model), key_weight, key_cotangent, bucket, sign_bits, momentum.reshape(flat), error.reshape(flat))
    return grad, momentum_new.reshape(momentum.shape), error_new.reshape(error.shape), update


def solution(mesh):
    in_specs = (
        P(("dp", "fsdp"), None),
        P(),
        P("fsdp", None),
        P(("dp", "fsdp"), None),
        P(None, "fsdp"),
        P(None, "fsdp"),
        P("fsdp", None, "dp"),
        P("fsdp", None, "dp"),
    )
    out_specs = (
        P(("dp", "fsdp"), None),
        P("fsdp", None, "dp"),
        P("fsdp", None, "dp"),
        P("fsdp", None),
    )
    return jax.shard_map(
        on_device, mesh=mesh, in_specs=in_specs, out_specs=out_specs, check_vma=False
    )
```

```python
import functools
import math

import jax
import jax.numpy as jnp
from jax import lax
from jax.experimental import pallas as pl
from jax.experimental.pallas import tpu as pltpu
from jax.sharding import PartitionSpec as P

ROWS = 5
NBB = 256
BLOCK = 128
EPS = 1e-05
DECAY = 0.9
THRESHOLD = 1.0
N = 16
BLK = 4
Z = 8
BF = jnp.bfloat16
F32 = jnp.float32
MESH = pl.DeviceIdType.MESH
PLAIN = (((1,), (0,)), ((), ()))
LAST = (((1,), (1,)), ((), ()))
FIRST = (((0,), (0,)), ((), ()))
DP_ORDER = [(1, d) for d in (4, 3, 5, 2, 6, 1, 7, 0)] + [(0, d) for d in (4, 3, 5, 2, 6, 1, 7)]


def dot(a, b, numbers):
    return lax.dot_general(a, b, numbers, preferred_element_type=F32)


def middle_three(first, second, third):
    return jnp.maximum(jnp.minimum(first, second), jnp.minimum(jnp.maximum(first, second), third))


def middle_five(items):
    upper_pair = jnp.minimum(jnp.maximum(items[0], items[1]), jnp.maximum(items[2], items[3]))
    lower_pair = jnp.maximum(jnp.minimum(items[0], items[1]), jnp.minimum(items[2], items[3]))
    return middle_three(items[4], upper_pair, lower_pair)


def split(values):
    upper = values.astype(BF)
    return upper, (values - upper.astype(F32)).astype(BF)


def kernel(
    scale,
    hs_hbm, gain_hbm, kw_hbm, cot_hbm, bucket_hbm, bits_hbm, mom_hbm, err_hbm,
    ig_hbm, mom_out, err_out, upd_hbm, fac_out,
    hs_v, hs_rx, cot_v, cot_rx, kw_v, ig_tx, ig_rx, acc, blk, blk2, sel, table_bf, rs_rx, e_all,
    e_mid, upd_v, gcol, inv_v, ublk, ublk2, sel_h, bucket_h, bits_h,
    gain_ref, bucket_ref, bits_ref, mom_ref, err_ref, mom_new, err_new, fac_v,
    load_sem, out_sem, cot_tx_s, cot_s, hs_tx_s, hs_s, ig_tx_s, ig_s, rs_tx_s, rs_s, ag_tx_s, ag_s, misc_s,
    shared_tx_s, shared_s, small_s,
):
    dp = lax.axis_index("dp")
    me = lax.axis_index("fsdp")
    xlo, z = dp // Z, dp % Z
    y, xhi, core = me // 4, (me // 2) % 2, me % 2
    tokens, width = hs_v.shape[1], hs_v.shape[2]

    def other(value):
        return value + 1 - 2 * (value % 2)

    def pick(kind, first, second):
        return first + kind * (second - first)

    def block_chip(kind, p):
        bx, by = p // 2, p % 2
        return (
            xhi + bx * pick(kind, 1 - 2 * xhi, 0),
            xlo + bx * (1 - 2 * xlo),
            y + by * (pick(kind, other(y), 3 - y) - y),
        )

    def held_slab(hi, lo, yy, kind, j):
        held_y = pick(kind, 3 - yy, other(yy)) if j else yy
        return held_y * 4 + pick(kind, hi, 1 - lo if j else lo) * 2 + kind

    def device(hi, lo, yy, zz, kind):
        return lo * Z + zz, yy * 4 + hi * 2 + kind

    def target(dc, p):
        kind = (core + dc) % 2
        return device(*block_chip(kind, p), z, kind)

    def target_slab(dc, p, j):
        kind = (core + dc) % 2
        return held_slab(*block_chip(kind, p), kind, j)

    def source(dc, p):
        return device(*block_chip(core, p), z, (core + dc) % 2)

    def dp_peer(dx, dz):
        return ((xlo + dx) % 2) * Z + (z + dz) % Z

    held = [held_slab(xhi, xlo, y, core, j) for j in range(2)]
    own_slab = held[0] == me
    unit = [pick(core, xlo, xhi), pick(core, xlo, 1 - xhi)]
    my_index = [unit[j] * Z + z for j in range(2)]

    def holder(j, dx, dz):
        u, zz = (xlo + dx) % 2, (z + Z - dz) % Z
        yy = pick(core, 3 - y, other(y)) if j else y
        hi, lo = (1 - u, 1 - xhi) if j else (u, xhi)
        return u * Z + zz, device(pick(core, xhi, hi), pick(core, u, lo), yy, zz, core)

    def owner(j, dx, dz):
        share_index = ((unit[j] + dx) % 2) * Z + (z + dz) % Z
        return share_index, (share_index, held[j])

    partner = [owner(j, 0, 0)[1] for j in range(2)]
    offsets = [(dc, p) for p in range(BLK) for dc in range(2) if (dc, p) != (0, 0)]

    hs_loads = [
        pltpu.make_async_copy(hs_hbm.at[:, pl.ds(s * width, width)], hs_v.at[s], load_sem.at[s]) for s in range(N)
    ]
    cot_load = pltpu.make_async_copy(cot_hbm, cot_v, misc_s.at[0])
    pairs = [(gain_hbm, gain_ref), (bucket_hbm, bucket_ref), (bits_hbm, bits_ref), (mom_hbm, mom_ref), (err_hbm, err_ref)]
    small_loads = [pltpu.make_async_copy(src, dst, small_s.at[k]) for k, (src, dst) in enumerate(pairs)]
    for copy in hs_loads:
        copy.start()
    cot_load.start()
    for copy in small_loads:
        copy.start()

    barrier = pltpu.get_barrier_semaphore()
    ready = 0
    for dc, p in offsets:
        pl.semaphore_signal(barrier, inc=1, device_id=source(dc, p), device_id_type=MESH)
        ready += 1
        if dc == 1 and p > 0:
            pl.semaphore_signal(barrier, inc=1, device_id=target(dc, p), device_id_type=MESH)
            ready += 1
    for off in DP_ORDER:
        pl.semaphore_signal(barrier, inc=1, device_id=(dp_peer(off[0], Z - off[1]), me), device_id_type=MESH)
        for j in range(2):
            pl.semaphore_signal(barrier, inc=1, device_id=holder(j, *off)[1], device_id_type=MESH)
        ready += 3

    for j in range(2):
        pl.semaphore_signal(barrier, inc=1, device_id=partner[j], device_id_type=MESH)
        ready += 1

    squares = jnp.zeros((tokens, BLOCK), F32)
    for s in range(N):
        hs_loads[s].wait()
        part = hs_v[s].astype(F32)
        part = part * part
        for q in range(width // BLOCK):
            squares = squares + part[:, q * BLOCK:(q + 1) * BLOCK]
    inverse = lax.rsqrt(jnp.sum(squares, axis=1, keepdims=True) / (N * width) + EPS)
    inv_v[...] = jnp.broadcast_to(inverse, (tokens, BLOCK))
    cot_load.wait()
    cot_rx[core] = (cot_v[...].astype(F32) * inverse).astype(BF)

    for copy in small_loads:
        copy.wait()
    pl.semaphore_wait(barrier, ready)

    def shared(j):
        return [(bucket_ref, bucket_h.at[j], 2 * j), (bits_ref, bits_h.at[j], 2 * j + 1), (kw_hbm, kw_v.at[j], 4 + j)]

    def to_partner(j, item):
        src, dst, k = item
        return pltpu.make_async_remote_copy(
            src_ref=src, dst_ref=dst, send_sem=shared_tx_s.at[k], recv_sem=shared_s.at[k],
            device_id=partner[j], device_id_type=MESH)

    def to_self(item):
        src, dst, k = item
        return pltpu.make_async_copy(src, dst, shared_s.at[k])

    def send_shared(pick_items):
        @pl.when(jnp.logical_not(own_slab))
        def _():
            for item in pick_items(shared(0)):
                to_partner(0, item).start()

        @pl.when(own_slab)
        def _():
            for item in pick_items(shared(0)):
                to_self(item).start()

        for item in pick_items(shared(1)):
            to_partner(1, item).start()

    send_shared(lambda items: items[:2])

    cot_sends = [
        pltpu.make_async_remote_copy(
            src_ref=cot_rx.at[core], dst_ref=cot_rx.at[2 * p + core], send_sem=cot_tx_s.at[k],
            recv_sem=cot_s.at[2 * p + core], device_id=target(dc, p), device_id_type=MESH)
        for k, (dc, p) in enumerate(offsets)
    ]
    for copy in cot_sends:
        copy.start()
    hs_sends = [
        pltpu.make_async_remote_copy(
            src_ref=hs_v.at[target_slab(dc, p, j)], dst_ref=hs_rx.at[j * 2 * BLK + 2 * p + core],
            send_sem=hs_tx_s.at[j * 2 * BLK + k],
            recv_sem=hs_s.at[j * 2 * BLK + 2 * p + core], device_id=target(dc, p), device_id_type=MESH)
        for j in range(2) for k, (dc, p) in enumerate(offsets)
    ]
    for copy in hs_sends:
        copy.start()
    own = [
        pltpu.make_async_copy(hs_v.at[held[j]], hs_rx.at[j * 2 * BLK + core], misc_s.at[1 + j]) for j in range(2)
    ]
    for copy in own:
        copy.start()
    send_shared(lambda items: items[2:])

    for j in range(2):
        gain_row = gain_ref[:, pl.ds(pl.multiple_of(held[j] * width, width), width)]
        gcol[j] = jnp.transpose(jnp.broadcast_to(gain_row * scale, (BLOCK, width)))

    def selectors(ids_ref, sign_ref, out):
        for j in range(ROWS):
            ids = jnp.broadcast_to(ids_ref[j:j + 1, :], (16, ids_ref.shape[1]))
            signs = jnp.broadcast_to((2 * sign_ref[j:j + 1, :] - 1).astype(F32), (16, ids_ref.shape[1]))
            row = lax.broadcasted_iota(jnp.int32, (16, ids_ref.shape[1]), 0)

            def fill(i, carry, j=j, ids=ids, signs=signs, row=row):
                start = pl.multiple_of(i * 16, 16)
                out[j, pl.ds(start, 16), :] = jnp.where(ids == row + i * 16, signs, 0.0).astype(BF)
                return carry

            lax.fori_loop(0, NBB // 16, fill, 0)

    acc[...] = jnp.zeros_like(acc)
    for j in range(2):
        for item in shared(j)[:2]:
            to_self(item).wait()
        selectors(bucket_h.at[j], bits_h.at[j], sel_h.at[j])
    selectors(bucket_ref, bits_ref, sel)
    for copy in own:
        copy.wait()

    def wait_slot(buffer, sem, slot):
        pltpu.make_async_remote_copy(
            src_ref=buffer.at[slot], dst_ref=buffer.at[slot], send_sem=misc_s.at[3], recv_sem=sem.at[slot],
            device_id=target(1, 0), device_id_type=MESH).wait_recv()

    parts = width // BLOCK
    share = NBB // N

    def half_weight_grad(j):
        def weight_grad(p, carry):
            if j == 0:
                wait_slot(cot_rx, cot_s, 2 * p + (core + 1) % 2)
            wait_slot(hs_rx, hs_s, j * 2 * BLK + 2 * p + (core + 1) % 2)

            @pl.when(p > 0)
            def _():
                if j == 0:
                    wait_slot(cot_rx, cot_s, 2 * p + core)
                wait_slot(hs_rx, hs_s, j * 2 * BLK + 2 * p + core)

            rows = hs_rx[pl.ds(j * 2 * BLK + p * 2, 2)].reshape(2 * tokens, width)
            cots = cot_rx[pl.ds(p * 2, 2)].reshape(2 * tokens, cot_rx.shape[2])
            acc[j] += dot(rows, cots, FIRST)
            return carry

        lax.fori_loop(0, BLK, weight_grad, 0)

        for q in range(parts):
            blk[pl.ds(q, width, stride=parts), :] = acc[j, :, q * BLOCK:(q + 1) * BLOCK] * gcol[j]

        def to_halves(i, carry):
            rows = pl.ds(pl.multiple_of(i * 256, 256), 256)
            upper, lower = split(blk[rows, :])
            blk2[rows, 0:BLOCK] = upper
            blk2[rows, BLOCK:] = lower
            return carry

        lax.fori_loop(0, blk.shape[0] // 256, to_halves, 0)

    def half_sketch(j, dx):
        rows = pl.ds(pl.multiple_of(((unit[j] + dx) % 2) * (NBB // 2), NBB // 2), NBB // 2)

        def sketch_row(i, carry):
            both = dot(sel_h[j, i, rows, :], blk2[...], PLAIN)
            table_bf[j, i, rows, :] = (both[:, :BLOCK] + both[:, BLOCK:]).astype(BF)
            return carry

        lax.fori_loop(0, ROWS, sketch_row, 0)

    def share_copy(j, k, off):
        index, place = owner(j, *off)
        return pltpu.make_async_remote_copy(
            src_ref=table_bf.at[j, :, pl.ds(pl.multiple_of(index * share, share), share), :],
            dst_ref=rs_rx.at[j * N + my_index[j]], send_sem=rs_tx_s.at[j * N + k],
            recv_sem=rs_s.at[j * N + my_index[j]],
            device_id=place, device_id_type=MESH)

    def ig_copy(j, k, dc, p):
        return pltpu.make_async_remote_copy(
            src_ref=ig_tx.at[j * 2 * BLK + 2 * p + (core + dc) % 2], dst_ref=ig_rx.at[held[j]],
            send_sem=ig_tx_s.at[j * 2 * BLK + k],
            recv_sem=ig_s.at[held[j]], device_id=source(dc, p), device_id_type=MESH)

    ig_sends = [ig_copy(j, k, dc, p) for j in range(2) for k, (dc, p) in enumerate(offsets)]
    ig_own = [
        pltpu.make_async_copy(ig_tx.at[j * 2 * BLK + core], ig_rx.at[held[j]], misc_s.at[4 + j]) for j in range(2)
    ]

    def send_input_grad(j):
        to_self(shared(j)[2]).wait()

        def input_grad(p, carry):
            rows = cot_rx[pl.ds(p * 2, 2)].reshape(2 * tokens, cot_rx.shape[2])
            product = dot(rows, kw_v[j], LAST).astype(BF)
            ig_tx[pl.ds(j * 2 * BLK + p * 2, 2)] = product.reshape(2, tokens, width)
            return carry

        lax.fori_loop(0, BLK, input_grad, 0)
        for k, (dc, p) in enumerate(offsets):
            ig_copy(j, k, dc, p).start()
        pltpu.make_async_copy(ig_tx.at[j * 2 * BLK + core], ig_rx.at[held[j]], misc_s.at[4 + j]).start()

    rs_sends = []
    for j in range(2):
        half_weight_grad(j)
        for dx in (1, 0):
            half_sketch(j, dx)
            sends = [share_copy(j, k, off) for k, off in enumerate(DP_ORDER) if off[0] == dx]
            for copy in sends:
                copy.start()
            rs_sends += sends
        if j == 1:
            rs_sends.append(share_copy(1, N - 1, (0, 0)))
            rs_sends[-1].start()
        else:
            @pl.when(jnp.logical_not(own_slab))
            def _():
                share_copy(0, N - 1, (0, 0)).start()

            @pl.when(own_slab)
            def _():
                pltpu.make_async_copy(
                    table_bf.at[0, :, pl.ds(pl.multiple_of(my_index[0] * share, share), share), :],
                    rs_rx.at[my_index[0]], rs_s.at[my_index[0]]).start()
                send_input_grad(0)

    for j in range(2):
        if j == 0:
            pl.when(jnp.logical_not(own_slab))(lambda: send_input_grad(0))
        else:
            send_input_grad(1)

    mine = pl.ds(pl.multiple_of(dp * share, share), share)
    total = jnp.zeros((ROWS, share, BLOCK), F32)
    for j in range(2):
        for off in DP_ORDER + [(0, 0)]:
            index = j * N + holder(j, *off)[0]
            pltpu.make_async_copy(rs_rx.at[index], rs_rx.at[index], rs_s.at[index]).wait()
            total = total + rs_rx[index].astype(F32)
    momentum_new = DECAY * mom_ref[...] + total
    error_sum = err_ref[...] + momentum_new
    mom_new[...] = momentum_new
    out_copies = [pltpu.make_async_copy(mom_new, mom_out, small_s.at[5])]
    out_copies[0].start()
    e_mid[...] = error_sum
    e_all[:, mine, :] = error_sum.astype(BF)
    ag_sends = []
    for k, off in enumerate(DP_ORDER):
        ag_sends.append(pltpu.make_async_remote_copy(
            src_ref=e_all.at[:, mine, :], dst_ref=e_all.at[:, mine, :], send_sem=ag_tx_s.at[k],
            recv_sem=ag_s.at[dp], device_id=(dp_peer(*off), me), device_id_type=MESH))
    for copy in ag_sends:
        copy.start()

    for copy in ig_own:
        copy.wait()

    def ig_store(slot):
        return pltpu.make_async_copy(ig_rx.at[slot], ig_hbm.at[slot], out_sem.at[slot])

    def row_sums(p, carry):
        for j in range(2):
            for dc in range(2):
                slot = target_slab(dc, p, j)
                if dc == 1:
                    wait_slot(ig_rx, ig_s, slot)
                else:
                    @pl.when(p > 0)
                    def _(slot=slot):
                        wait_slot(ig_rx, ig_s, slot)

                ig_store(slot).start()
                gains = gain_ref[:, pl.ds(pl.multiple_of(slot * width, width), width)]
                product = ig_rx[slot].astype(F32) * hs_v[slot].astype(F32) * gains
                for q in range(parts):
                    carry = carry + product[:, q * BLOCK:(q + 1) * BLOCK]
        return carry

    sums = lax.fori_loop(0, BLK, row_sums, jnp.zeros((tokens, BLOCK), F32))
    mean_term = jnp.sum(sums, axis=1, keepdims=True) / (N * width)
    inverse = inv_v[...]
    fac_v[...] = inverse * inverse * mean_term
    out_copies.append(pltpu.make_async_copy(fac_v, fac_out, small_s.at[7]))
    out_copies[-1].start()

    for off in DP_ORDER:
        index = dp_peer(*off)
        theirs = pl.ds(pl.multiple_of(index * share, share), share)
        pltpu.make_async_remote_copy(
            src_ref=e_all.at[:, theirs, :], dst_ref=e_all.at[:, theirs, :], send_sem=misc_s.at[3],
            recv_sem=ag_s.at[index], device_id=(index, me), device_id_type=MESH).wait_recv()

    def estimate(i, carry):
        start = pl.multiple_of(i * 512, 512)
        reads = [dot(e_all[j], sel[j, :, pl.ds(start, 512)], FIRST) for j in range(ROWS)]
        middle = middle_five(reads)
        update = jnp.transpose(middle - jnp.clip(middle, -THRESHOLD, THRESHOLD))
        rows = pl.ds(start, 512)
        ublk[rows, :] = update
        upper, lower = split(update)
        ublk2[rows, 0:BLOCK] = upper
        ublk2[rows, BLOCK:] = lower
        return carry

    lax.fori_loop(0, ublk.shape[0] // 512, estimate, 0)
    for q in range(parts):
        upd_v[:, q * BLOCK:(q + 1) * BLOCK] = ublk[pl.ds(q, width, stride=parts), :]
    upd_store = pltpu.make_async_copy(upd_v, upd_hbm, misc_s.at[6])
    upd_store.start()
    selected = sel[:, mine, :].reshape(ROWS * share, sel.shape[2])
    both = dot(selected, ublk2[...], PLAIN)
    err_new[...] = e_mid[...] - (both[:, :BLOCK] + both[:, BLOCK:]).reshape(ROWS, share, BLOCK)

    out_copies.append(pltpu.make_async_copy(err_new, err_out, small_s.at[6]))
    out_copies[-1].start()

    for copy in cot_sends + hs_sends + ig_sends + rs_sends + ag_sends:
        copy.wait_send()

    for item in shared(1):
        to_partner(1, item).wait_send()

    @pl.when(jnp.logical_not(own_slab))
    def _():
        for item in shared(0):
            to_partner(0, item).wait_send()
        share_copy(0, N - 1, (0, 0)).wait_send()

    for slot in range(N):
        ig_store(slot).wait()
    upd_store.wait()
    for copy in out_copies:
        copy.wait()


def results_kernel(
    ig_hbm, hs_hbm, gain_hbm, fac_hbm, mom_hbm, err_hbm, upd_hbm,
    grad_hbm, mom_out, err_out, upd_out,
    ig_v, hs_v, out_v, gain_v, fac_v, mom_v, err_v, upd_v, in_sem, hs_sem, out_sem, pass_in, pass_out,
):
    count = in_sem.shape[0]
    height = hs_v.shape[0] // count
    width = ig_v.shape[2]

    def band(s):
        return pl.ds(pl.multiple_of(s * height, height), height)

    def load(s):
        return (
            pltpu.make_async_copy(ig_hbm.at[:, band(s), :], ig_v.at[:, band(s), :], in_sem.at[s]),
            pltpu.make_async_copy(hs_hbm.at[band(s)], hs_v.at[band(s)], hs_sem.at[s]),
        )

    def store(s):
        return pltpu.make_async_copy(out_v.at[band(s)], grad_hbm.at[band(s)], out_sem.at[s])

    small = [
        pltpu.make_async_copy(gain_hbm, gain_v, pass_in.at[3]), pltpu.make_async_copy(fac_hbm, fac_v, pass_in.at[4])
    ]
    for copy in small:
        copy.start()
    for s in range(count):
        for copy in load(s):
            copy.start()
    passed = [(mom_hbm, mom_v, mom_out), (err_hbm, err_v, err_out), (upd_hbm, upd_v, upd_out)]
    arrivals = [pltpu.make_async_copy(src, mid, pass_in.at[k]) for k, (src, mid, _) in enumerate(passed)]
    departures = [pltpu.make_async_copy(mid, dst, pass_out.at[k]) for k, (_, mid, dst) in enumerate(passed)]
    for copy in arrivals:
        copy.start()
    for copy in small:
        copy.wait()

    def hidden(s, carry):
        for copy in load(s):
            copy.wait()
        factor = fac_v[band(s), :]
        for t in range(N):
            for q in range(width // BLOCK):
                inner = slice(q * BLOCK, (q + 1) * BLOCK)
                outer = slice(t * width + q * BLOCK, t * width + (q + 1) * BLOCK)
                out_v[band(s), outer] = (
                    ig_v[t, band(s), inner].astype(F32) * gain_v[:, outer] - hs_v[band(s), outer].astype(F32) * factor
                ).astype(BF)
        store(s).start()
        return carry

    lax.fori_loop(0, count, hidden, 0)
    for arrival, departure in zip(arrivals, departures):
        arrival.wait()
        departure.start()
    for s in range(count):
        store(s).wait()
    for departure in departures:
        departure.wait()


def on_device(hidden_states, gain, key_weight, key_cotangent, bucket, sign_bits, momentum, error):
    tokens, model = hidden_states.shape
    width, keys = key_weight.shape
    count = bucket.shape[1]
    scale = 1.0 / math.sqrt(tokens * N) / N
    any_spec = pl.BlockSpec(memory_space=pl.ANY)
    dma = pltpu.SemaphoreType.DMA
    share = momentum.shape[2] // BLOCK
    flat = (ROWS, share, BLOCK)
    gain_row = gain.reshape(1, model)
    returned, momentum_new, error_new, update, factor = pl.pallas_call(
        functools.partial(kernel, scale),
        out_shape=(
            jax.ShapeDtypeStruct((N, tokens, width), BF),
            jax.ShapeDtypeStruct((ROWS, share, BLOCK), F32),
            jax.ShapeDtypeStruct((ROWS, share, BLOCK), F32),
            jax.ShapeDtypeStruct((width, keys), F32),
            jax.ShapeDtypeStruct((tokens, BLOCK), F32),
        ),
        in_specs=[any_spec] * 8,
        out_specs=(any_spec,) * 5,
        scratch_shapes=[
            pltpu.VMEM((N, tokens, width), BF),
            pltpu.VMEM((N, tokens, width), BF),
            pltpu.VMEM((tokens, keys), BF),
            pltpu.VMEM((2 * BLK, tokens, keys), BF),
            pltpu.VMEM((2, width, keys), BF),
            pltpu.VMEM((N, tokens, width), BF),
            pltpu.VMEM((N, tokens, width), BF),
            pltpu.VMEM((2, width, keys), F32),
            pltpu.VMEM((count, BLOCK), F32),
            pltpu.VMEM((count, 2 * BLOCK), BF),
            pltpu.VMEM((ROWS, NBB, count), BF),
            pltpu.VMEM((2, ROWS, NBB, BLOCK), BF),
            pltpu.VMEM((2 * N, ROWS, share, BLOCK), BF),
            pltpu.VMEM((ROWS, NBB, BLOCK), BF),
            pltpu.VMEM((ROWS, share, BLOCK), F32),
            pltpu.VMEM((width, keys), F32),
            pltpu.VMEM((2, width, BLOCK), F32),
            pltpu.VMEM((tokens, BLOCK), F32),
            pltpu.VMEM((count, BLOCK), F32),
            pltpu.VMEM((count, 2 * BLOCK), BF),
            pltpu.VMEM((2, ROWS, NBB, count), BF),
            pltpu.VMEM((2,) + bucket.shape, jnp.int32),
            pltpu.VMEM((2,) + bucket.shape, jnp.int32),
            pltpu.VMEM((1, model), F32),
            pltpu.VMEM(bucket.shape, jnp.int32),
            pltpu.VMEM(bucket.shape, jnp.int32),
            pltpu.VMEM(flat, F32),
            pltpu.VMEM(flat, F32),
            pltpu.VMEM(flat, F32),
            pltpu.VMEM(flat, F32),
            pltpu.VMEM((tokens, BLOCK), F32),
            dma((N,)), dma((N,)), dma((8,)), dma((8,)), dma((N,)), dma((N,)), dma((N,)), dma((N,)),
            dma((2 * N,)), dma((2 * N,)), dma((N,)), dma((N,)), dma((8,)), dma((8,)), dma((8,)), dma((8,)),
        ],
        compiler_params=pltpu.CompilerParams(
            collective_id=0, has_side_effects=True, vmem_limit_bytes=60 * 1024 * 1024),
        name="step",
    )(hidden_states, gain_row, key_weight, key_cotangent, bucket, sign_bits, momentum.reshape(flat), error.reshape(flat))
    grad, momentum_new, error_new, update = pl.pallas_call(
        results_kernel,
        out_shape=(
            jax.ShapeDtypeStruct((tokens, model), BF),
            jax.ShapeDtypeStruct(flat, F32),
            jax.ShapeDtypeStruct(flat, F32),
            jax.ShapeDtypeStruct((width, keys), F32),
        ),
        in_specs=[any_spec] * 7,
        out_specs=(any_spec,) * 4,
        scratch_shapes=[
            pltpu.VMEM((N, tokens, width), BF),
            pltpu.VMEM((tokens, model), BF),
            pltpu.VMEM((tokens, model), BF),
            pltpu.VMEM((1, model), F32),
            pltpu.VMEM((tokens, BLOCK), F32),
            pltpu.VMEM(flat, F32),
            pltpu.VMEM(flat, F32),
            pltpu.VMEM((width, keys), F32),
            dma((8,)), dma((8,)), dma((8,)), dma((5,)), dma((3,)),
        ],
        compiler_params=pltpu.CompilerParams(vmem_limit_bytes=60 * 1024 * 1024),
        name="tail",
    )(returned, hidden_states, gain_row, factor, momentum_new, error_new, update)
    return grad, momentum_new.reshape(momentum.shape), error_new.reshape(error.shape), update


def solution(mesh):
    in_specs = (
        P(("dp", "fsdp"), None),
        P(),
        P("fsdp", None),
        P(("dp", "fsdp"), None),
        P(None, "fsdp"),
        P(None, "fsdp"),
        P("fsdp", None, "dp"),
        P("fsdp", None, "dp"),
    )
    out_specs = (
        P(("dp", "fsdp"), None),
        P("fsdp", None, "dp"),
        P("fsdp", None, "dp"),
        P("fsdp", None),
    )
    return jax.shard_map(
        on_device, mesh=mesh, in_specs=in_specs, out_specs=out_specs, check_vma=False
    )
```

```python
import functools
import math

import jax
import jax.numpy as jnp
from jax import lax
from jax.experimental import pallas as pl
from jax.experimental.pallas import tpu as pltpu
from jax.sharding import PartitionSpec as P

ROWS = 5
NBB = 256
BLOCK = 128
EPS = 1e-05
DECAY = 0.9
THRESHOLD = 1.0
N = 16
BLK = 4
Z = 8
BF = jnp.bfloat16
F32 = jnp.float32
MESH = pl.DeviceIdType.MESH
PLAIN = (((1,), (0,)), ((), ()))
LAST = (((1,), (1,)), ((), ()))
FIRST = (((0,), (0,)), ((), ()))
DP_ORDER = [(1, d) for d in (4, 3, 5, 2, 6, 1, 7, 0)] + [(0, d) for d in (4, 3, 5, 2, 6, 1, 7)]


def dot(a, b, numbers):
    return lax.dot_general(a, b, numbers, preferred_element_type=F32)


def middle_three(first, second, third):
    return jnp.maximum(jnp.minimum(first, second), jnp.minimum(jnp.maximum(first, second), third))


def middle_five(items):
    upper_pair = jnp.minimum(jnp.maximum(items[0], items[1]), jnp.maximum(items[2], items[3]))
    lower_pair = jnp.maximum(jnp.minimum(items[0], items[1]), jnp.minimum(items[2], items[3]))
    return middle_three(items[4], upper_pair, lower_pair)


def split(values):
    upper = values.astype(BF)
    return upper, (values - upper.astype(F32)).astype(BF)


def kernel(
    scale,
    hs_hbm, gain_hbm, kw_hbm, cot_hbm, bucket_hbm, bits_hbm, mom_hbm, err_hbm,
    ig_hbm, mom_out, err_out, upd_hbm, fac_out,
    hs_v, hs_rx, cot_v, cot_rx, kw_v, ig_tx, ig_rx, acc, blk, blk2, sel, table_bf, rs_rx, e_all,
    e_mid, upd_v, gcol, inv_v, ublk, ublk2, sel_h, bucket_h, bits_h,
    gain_ref, bucket_ref, bits_ref, mom_ref, err_ref, mom_new, err_new, fac_v, e_cols,
    load_sem, out_sem, cot_tx_s, cot_s, hs_tx_s, hs_s, ig_tx_s, ig_s, rs_tx_s, rs_s, ag_tx_s, ag_s, misc_s,
    shared_tx_s, shared_s, small_s,
):
    dp = lax.axis_index("dp")
    me = lax.axis_index("fsdp")
    xlo, z = dp // Z, dp % Z
    y, xhi, core = me // 4, (me // 2) % 2, me % 2
    tokens, width = hs_v.shape[1], hs_v.shape[2]

    def other(value):
        return value + 1 - 2 * (value % 2)

    def pick(kind, first, second):
        return first + kind * (second - first)

    def block_chip(kind, p):
        bx, by = p // 2, p % 2
        return (
            xhi + bx * pick(kind, 1 - 2 * xhi, 0),
            xlo + bx * (1 - 2 * xlo),
            y + by * (pick(kind, other(y), 3 - y) - y),
        )

    def held_slab(hi, lo, yy, kind, j):
        held_y = pick(kind, 3 - yy, other(yy)) if j else yy
        return held_y * 4 + pick(kind, hi, 1 - lo if j else lo) * 2 + kind

    def device(hi, lo, yy, zz, kind):
        return lo * Z + zz, yy * 4 + hi * 2 + kind

    def target(dc, p):
        kind = (core + dc) % 2
        return device(*block_chip(kind, p), z, kind)

    def target_slab(dc, p, j):
        kind = (core + dc) % 2
        return held_slab(*block_chip(kind, p), kind, j)

    def source(dc, p):
        return device(*block_chip(core, p), z, (core + dc) % 2)

    def dp_peer(dx, dz):
        return ((xlo + dx) % 2) * Z + (z + dz) % Z

    held = [held_slab(xhi, xlo, y, core, j) for j in range(2)]
    own_slab = held[0] == me
    unit = [pick(core, xlo, xhi), pick(core, xlo, 1 - xhi)]
    my_index = [unit[j] * Z + z for j in range(2)]

    def holder(j, dx, dz):
        u, zz = (xlo + dx) % 2, (z + Z - dz) % Z
        yy = pick(core, 3 - y, other(y)) if j else y
        hi, lo = (1 - u, 1 - xhi) if j else (u, xhi)
        return u * Z + zz, device(pick(core, xhi, hi), pick(core, u, lo), yy, zz, core)

    def owner(j, dx, dz):
        share_index = ((unit[j] + dx) % 2) * Z + (z + dz) % Z
        return share_index, (share_index, held[j])

    partner = [owner(j, 0, 0)[1] for j in range(2)]
    offsets = [(dc, p) for p in range(BLK) for dc in range(2) if (dc, p) != (0, 0)]

    hs_loads = [
        pltpu.make_async_copy(hs_hbm.at[:, pl.ds(s * width, width)], hs_v.at[s], load_sem.at[s]) for s in range(N)
    ]
    cot_load = pltpu.make_async_copy(cot_hbm, cot_v, misc_s.at[0])
    pairs = [(gain_hbm, gain_ref), (bucket_hbm, bucket_ref), (bits_hbm, bits_ref), (mom_hbm, mom_ref), (err_hbm, err_ref)]
    small_loads = [pltpu.make_async_copy(src, dst, small_s.at[k]) for k, (src, dst) in enumerate(pairs)]
    barrier = pltpu.get_barrier_semaphore()
    ready = 0
    for dc, p in offsets:
        pl.semaphore_signal(barrier, inc=1, device_id=source(dc, p), device_id_type=MESH)
        ready += 1
        if dc == 1 and p > 0:
            pl.semaphore_signal(barrier, inc=1, device_id=target(dc, p), device_id_type=MESH)
            ready += 1
    for off in DP_ORDER:
        pl.semaphore_signal(barrier, inc=1, device_id=(dp_peer(off[0], Z - off[1]), me), device_id_type=MESH)
        for j in range(2):
            pl.semaphore_signal(barrier, inc=1, device_id=holder(j, *off)[1], device_id_type=MESH)
        ready += 3

    for j in range(2):
        pl.semaphore_signal(barrier, inc=1, device_id=partner[j], device_id_type=MESH)
        ready += 1

    for copy in hs_loads:
        copy.start()
    cot_load.start()
    for copy in small_loads:
        copy.start()

    squares = jnp.zeros((tokens, BLOCK), F32)
    for s in range(N):
        hs_loads[s].wait()
        part = hs_v[s].astype(F32)
        part = part * part
        for q in range(width // BLOCK):
            squares = squares + part[:, q * BLOCK:(q + 1) * BLOCK]
    inverse = lax.rsqrt(jnp.sum(squares, axis=1, keepdims=True) / (N * width) + EPS)
    inv_v[...] = jnp.broadcast_to(inverse, (tokens, BLOCK))
    cot_load.wait()
    cot_rx[core] = (cot_v[...].astype(F32) * inverse).astype(BF)

    for copy in small_loads:
        copy.wait()
    pl.semaphore_wait(barrier, ready)

    def shared(j):
        return [(bucket_ref, bucket_h.at[j], 2 * j), (bits_ref, bits_h.at[j], 2 * j + 1), (kw_hbm, kw_v.at[j], 4 + j)]

    def to_partner(j, item):
        src, dst, k = item
        return pltpu.make_async_remote_copy(
            src_ref=src, dst_ref=dst, send_sem=shared_tx_s.at[k], recv_sem=shared_s.at[k],
            device_id=partner[j], device_id_type=MESH)

    def to_self(item):
        src, dst, k = item
        return pltpu.make_async_copy(src, dst, shared_s.at[k])

    def send_shared(pick_items):
        @pl.when(jnp.logical_not(own_slab))
        def _():
            for item in pick_items(shared(0)):
                to_partner(0, item).start()

        @pl.when(own_slab)
        def _():
            for item in pick_items(shared(0)):
                to_self(item).start()

        for item in pick_items(shared(1)):
            to_partner(1, item).start()

    send_shared(lambda items: items[:2])

    cot_sends = [
        pltpu.make_async_remote_copy(
            src_ref=cot_rx.at[core], dst_ref=cot_rx.at[2 * p + core], send_sem=cot_tx_s.at[k],
            recv_sem=cot_s.at[2 * p + core], device_id=target(dc, p), device_id_type=MESH)
        for k, (dc, p) in enumerate(offsets)
    ]
    for copy in cot_sends:
        copy.start()
    hs_sends = [
        pltpu.make_async_remote_copy(
            src_ref=hs_v.at[target_slab(dc, p, j)], dst_ref=hs_rx.at[j * 2 * BLK + 2 * p + core],
            send_sem=hs_tx_s.at[j * 2 * BLK + k],
            recv_sem=hs_s.at[j * 2 * BLK + 2 * p + core], device_id=target(dc, p), device_id_type=MESH)
        for j in range(2) for k, (dc, p) in enumerate(offsets)
    ]
    for copy in hs_sends:
        copy.start()
    own = [
        pltpu.make_async_copy(hs_v.at[held[j]], hs_rx.at[j * 2 * BLK + core], misc_s.at[1 + j]) for j in range(2)
    ]
    for copy in own:
        copy.start()
    send_shared(lambda items: items[2:])

    for j in range(2):
        gain_row = gain_ref[:, pl.ds(pl.multiple_of(held[j] * width, width), width)]
        gcol[j] = jnp.transpose(jnp.broadcast_to(gain_row * scale, (BLOCK, width)))

    def selectors(ids_ref, sign_ref, out):
        for j in range(ROWS):
            ids = jnp.broadcast_to(ids_ref[j:j + 1, :], (16, ids_ref.shape[1]))
            signs = jnp.broadcast_to((2 * sign_ref[j:j + 1, :] - 1).astype(F32), (16, ids_ref.shape[1]))
            row = lax.broadcasted_iota(jnp.int32, (16, ids_ref.shape[1]), 0)

            def fill(i, carry, j=j, ids=ids, signs=signs, row=row):
                start = pl.multiple_of(i * 16, 16)
                out[j, pl.ds(start, 16), :] = jnp.where(ids == row + i * 16, signs, 0.0).astype(BF)
                return carry

            lax.fori_loop(0, NBB // 16, fill, 0)

    acc[...] = jnp.zeros_like(acc)
    for j in range(2):
        for item in shared(j)[:2]:
            to_self(item).wait()
        selectors(bucket_h.at[j], bits_h.at[j], sel_h.at[j])
    selectors(bucket_ref, bits_ref, sel)
    for copy in own:
        copy.wait()

    def wait_slot(buffer, sem, slot):
        pltpu.make_async_remote_copy(
            src_ref=buffer.at[slot], dst_ref=buffer.at[slot], send_sem=misc_s.at[3], recv_sem=sem.at[slot],
            device_id=target(1, 0), device_id_type=MESH).wait_recv()

    parts = width // BLOCK
    share = NBB // N

    def half_weight_grad(j):
        def weight_grad(p, carry):
            if j == 0:
                wait_slot(cot_rx, cot_s, 2 * p + (core + 1) % 2)
            wait_slot(hs_rx, hs_s, j * 2 * BLK + 2 * p + (core + 1) % 2)

            @pl.when(p > 0)
            def _():
                if j == 0:
                    wait_slot(cot_rx, cot_s, 2 * p + core)
                wait_slot(hs_rx, hs_s, j * 2 * BLK + 2 * p + core)

            rows = hs_rx[pl.ds(j * 2 * BLK + p * 2, 2)].reshape(2 * tokens, width)
            cots = cot_rx[pl.ds(p * 2, 2)].reshape(2 * tokens, cot_rx.shape[2])
            acc[j] += dot(rows, cots, FIRST)
            return carry

        lax.fori_loop(0, BLK, weight_grad, 0)

        for q in range(parts):
            blk[pl.ds(q, width, stride=parts), :] = acc[j, :, q * BLOCK:(q + 1) * BLOCK] * gcol[j]

        def to_halves(i, carry):
            rows = pl.ds(pl.multiple_of(i * 256, 256), 256)
            upper, lower = split(blk[rows, :])
            blk2[rows, 0:BLOCK] = upper
            blk2[rows, BLOCK:] = lower
            return carry

        lax.fori_loop(0, blk.shape[0] // 256, to_halves, 0)

    def half_sketch(j, dx):
        first = ((unit[j] + dx) % 2) * (N // 2)
        rows = pl.ds(pl.multiple_of(first * share, NBB // 2), NBB // 2)

        def sketch_row(i, carry):
            both = dot(sel_h[j, i, rows, :], blk2[...], PLAIN)
            table_bf[j, pl.ds(first, N // 2), i] = (
                (both[:, :BLOCK] + both[:, BLOCK:]).astype(BF).reshape(N // 2, share, BLOCK))
            return carry

        lax.fori_loop(0, ROWS, sketch_row, 0)

    def share_copy(j, k, off):
        index, place = owner(j, *off)
        return pltpu.make_async_remote_copy(
            src_ref=table_bf.at[j, index],
            dst_ref=rs_rx.at[j * N + my_index[j]], send_sem=rs_tx_s.at[j * N + k],
            recv_sem=rs_s.at[j * N + my_index[j]],
            device_id=place, device_id_type=MESH)

    def ig_copy(j, k, dc, p):
        return pltpu.make_async_remote_copy(
            src_ref=ig_tx.at[j * 2 * BLK + 2 * p + (core + dc) % 2], dst_ref=ig_rx.at[held[j]],
            send_sem=ig_tx_s.at[j * 2 * BLK + k],
            recv_sem=ig_s.at[held[j]], device_id=source(dc, p), device_id_type=MESH)

    ig_sends = [ig_copy(j, k, dc, p) for j in range(2) for k, (dc, p) in enumerate(offsets)]
    ig_own = [
        pltpu.make_async_copy(ig_tx.at[j * 2 * BLK + core], ig_rx.at[held[j]], misc_s.at[4 + j]) for j in range(2)
    ]

    def send_input_grad(j):
        to_self(shared(j)[2]).wait()

        def input_grad(p, carry):
            rows = cot_rx[pl.ds(p * 2, 2)].reshape(2 * tokens, cot_rx.shape[2])
            product = dot(rows, kw_v[j], LAST).astype(BF)
            ig_tx[pl.ds(j * 2 * BLK + p * 2, 2)] = product.reshape(2, tokens, width)
            return carry

        lax.fori_loop(0, BLK, input_grad, 0)
        for k, (dc, p) in enumerate(offsets):
            ig_copy(j, k, dc, p).start()
        pltpu.make_async_copy(ig_tx.at[j * 2 * BLK + core], ig_rx.at[held[j]], misc_s.at[4 + j]).start()

    rs_sends = []
    for j in range(2):
        half_weight_grad(j)
        for dx in (1, 0):
            half_sketch(j, dx)
            sends = [share_copy(j, k, off) for k, off in enumerate(DP_ORDER) if off[0] == dx]
            for copy in sends:
                copy.start()
            rs_sends += sends
        if j == 1:
            rs_sends.append(share_copy(1, N - 1, (0, 0)))
            rs_sends[-1].start()
        else:
            @pl.when(jnp.logical_not(own_slab))
            def _():
                share_copy(0, N - 1, (0, 0)).start()

            @pl.when(own_slab)
            def _():
                pltpu.make_async_copy(
                    table_bf.at[0, my_index[0]], rs_rx.at[my_index[0]], rs_s.at[my_index[0]]).start()
                send_input_grad(0)

    for j in range(2):
        if j == 0:
            pl.when(jnp.logical_not(own_slab))(lambda: send_input_grad(0))
        else:
            send_input_grad(1)

    mine = pl.ds(pl.multiple_of(dp * share, share), share)
    total = jnp.zeros((ROWS, share, BLOCK), F32)
    for j in range(2):
        for off in DP_ORDER + [(0, 0)]:
            index = j * N + holder(j, *off)[0]
            pltpu.make_async_copy(rs_rx.at[index], rs_rx.at[index], rs_s.at[index]).wait()
            total = total + rs_rx[index].astype(F32)
    momentum_new = DECAY * mom_ref[...] + total
    error_sum = err_ref[...] + momentum_new
    mom_new[...] = momentum_new
    out_copies = [pltpu.make_async_copy(mom_new, mom_out, small_s.at[5])]
    out_copies[0].start()
    e_mid[...] = error_sum
    e_all[dp] = error_sum.astype(BF)
    ag_sends = []
    for k, off in enumerate(DP_ORDER):
        ag_sends.append(pltpu.make_async_remote_copy(
            src_ref=e_all.at[dp], dst_ref=e_all.at[dp], send_sem=ag_tx_s.at[k],
            recv_sem=ag_s.at[dp], device_id=(dp_peer(*off), me), device_id_type=MESH))
    for copy in ag_sends:
        copy.start()

    for copy in ig_own:
        copy.wait()

    def ig_store(slot):
        return pltpu.make_async_copy(ig_rx.at[slot], ig_hbm.at[slot], out_sem.at[slot])

    def row_sums(p, carry):
        for j in range(2):
            for dc in range(2):
                slot = target_slab(dc, p, j)
                if dc == 1:
                    wait_slot(ig_rx, ig_s, slot)
                else:
                    @pl.when(p > 0)
                    def _(slot=slot):
                        wait_slot(ig_rx, ig_s, slot)

                ig_store(slot).start()
                gains = gain_ref[:, pl.ds(pl.multiple_of(slot * width, width), width)]
                product = ig_rx[slot].astype(F32) * hs_v[slot].astype(F32) * gains
                for q in range(parts):
                    carry = carry + product[:, q * BLOCK:(q + 1) * BLOCK]
        return carry

    sums = lax.fori_loop(0, BLK, row_sums, jnp.zeros((tokens, BLOCK), F32))
    mean_term = jnp.sum(sums, axis=1, keepdims=True) / (N * width)
    inverse = inv_v[...]
    fac_v[...] = inverse * inverse * mean_term
    out_copies.append(pltpu.make_async_copy(fac_v, fac_out, small_s.at[7]))
    out_copies[-1].start()

    for off in DP_ORDER:
        index = dp_peer(*off)
        pltpu.make_async_remote_copy(
            src_ref=e_all.at[index], dst_ref=e_all.at[index], send_sem=misc_s.at[3],
            recv_sem=ag_s.at[index], device_id=(index, me), device_id_type=MESH).wait_recv()

    for j in range(ROWS):
        e_cols[j] = jnp.transpose(e_all[:, j].reshape(NBB, BLOCK))

    def estimate(i, carry):
        start = pl.multiple_of(i * 512, 512)
        reads = [dot(e_cols[j], sel[j, :, pl.ds(start, 512)], PLAIN) for j in range(ROWS)]
        middle = middle_five(reads)
        update = jnp.transpose(middle - jnp.clip(middle, -THRESHOLD, THRESHOLD))
        rows = pl.ds(start, 512)
        ublk[rows, :] = update
        upper, lower = split(update)
        ublk2[rows, 0:BLOCK] = upper
        ublk2[rows, BLOCK:] = lower
        return carry

    lax.fori_loop(0, ublk.shape[0] // 512, estimate, 0, unroll=True)
    for q in range(parts):
        upd_v[:, q * BLOCK:(q + 1) * BLOCK] = ublk[pl.ds(q, width, stride=parts), :]
    upd_store = pltpu.make_async_copy(upd_v, upd_hbm, misc_s.at[6])
    upd_store.start()
    selected = sel[:, mine, :].reshape(ROWS * share, sel.shape[2])
    both = dot(selected, ublk2[...], PLAIN)
    err_new[...] = e_mid[...] - (both[:, :BLOCK] + both[:, BLOCK:]).reshape(ROWS, share, BLOCK)

    out_copies.append(pltpu.make_async_copy(err_new, err_out, small_s.at[6]))
    out_copies[-1].start()

    for copy in cot_sends + hs_sends + ig_sends + rs_sends + ag_sends:
        copy.wait_send()

    for item in shared(1):
        to_partner(1, item).wait_send()

    @pl.when(jnp.logical_not(own_slab))
    def _():
        for item in shared(0):
            to_partner(0, item).wait_send()
        share_copy(0, N - 1, (0, 0)).wait_send()

    for slot in range(N):
        ig_store(slot).wait()
    upd_store.wait()
    for copy in out_copies:
        copy.wait()


def results_kernel(
    ig_hbm, hs_hbm, gain_hbm, fac_hbm, mom_hbm, err_hbm, upd_hbm,
    grad_hbm, mom_out, err_out, upd_out,
    ig_v, hs_v, out_v, gain_v, fac_v, mom_v, err_v, upd_v, in_sem, hs_sem, out_sem, pass_in, pass_out,
):
    count = in_sem.shape[0]
    height = hs_v.shape[0] // count
    width = ig_v.shape[2]

    def band(s):
        return pl.ds(pl.multiple_of(s * height, height), height)

    def load(s):
        return (
            pltpu.make_async_copy(ig_hbm.at[:, band(s), :], ig_v.at[:, band(s), :], in_sem.at[s]),
            pltpu.make_async_copy(hs_hbm.at[band(s)], hs_v.at[band(s)], hs_sem.at[s]),
        )

    def store(s):
        return pltpu.make_async_copy(out_v.at[band(s)], grad_hbm.at[band(s)], out_sem.at[s])

    small = [
        pltpu.make_async_copy(gain_hbm, gain_v, pass_in.at[3]), pltpu.make_async_copy(fac_hbm, fac_v, pass_in.at[4])
    ]
    for copy in small:
        copy.start()
    for s in range(count):
        for copy in load(s):
            copy.start()
    passed = [(mom_hbm, mom_v, mom_out), (err_hbm, err_v, err_out), (upd_hbm, upd_v, upd_out)]
    arrivals = [pltpu.make_async_copy(src, mid, pass_in.at[k]) for k, (src, mid, _) in enumerate(passed)]
    departures = [pltpu.make_async_copy(mid, dst, pass_out.at[k]) for k, (_, mid, dst) in enumerate(passed)]
    for copy in arrivals:
        copy.start()
    for copy in small:
        copy.wait()

    def hidden(s, carry):
        for copy in load(s):
            copy.wait()
        factor = fac_v[band(s), :]
        for t in range(N):
            for q in range(width // BLOCK):
                inner = slice(q * BLOCK, (q + 1) * BLOCK)
                outer = slice(t * width + q * BLOCK, t * width + (q + 1) * BLOCK)
                out_v[band(s), outer] = (
                    ig_v[t, band(s), inner].astype(F32) * gain_v[:, outer] - hs_v[band(s), outer].astype(F32) * factor
                ).astype(BF)
        store(s).start()
        return carry

    lax.fori_loop(0, count, hidden, 0)
    for arrival, departure in zip(arrivals, departures):
        arrival.wait()
        departure.start()
    for s in range(count):
        store(s).wait()
    for departure in departures:
        departure.wait()


def on_device(hidden_states, gain, key_weight, key_cotangent, bucket, sign_bits, momentum, error):
    tokens, model = hidden_states.shape
    width, keys = key_weight.shape
    count = bucket.shape[1]
    scale = 1.0 / math.sqrt(tokens * N) / N
    any_spec = pl.BlockSpec(memory_space=pl.ANY)
    dma = pltpu.SemaphoreType.DMA
    share = momentum.shape[2] // BLOCK
    flat = (ROWS, share, BLOCK)
    gain_row = gain.reshape(1, model)
    returned, momentum_new, error_new, update, factor = pl.pallas_call(
        functools.partial(kernel, scale),
        out_shape=(
            jax.ShapeDtypeStruct((N, tokens, width), BF),
            jax.ShapeDtypeStruct((ROWS, share, BLOCK), F32),
            jax.ShapeDtypeStruct((ROWS, share, BLOCK), F32),
            jax.ShapeDtypeStruct((width, keys), F32),
            jax.ShapeDtypeStruct((tokens, BLOCK), F32),
        ),
        in_specs=[any_spec] * 8,
        out_specs=(any_spec,) * 5,
        scratch_shapes=[
            pltpu.VMEM((N, tokens, width), BF),
            pltpu.VMEM((N, tokens, width), BF),
            pltpu.VMEM((tokens, keys), BF),
            pltpu.VMEM((2 * BLK, tokens, keys), BF),
            pltpu.VMEM((2, width, keys), BF),
            pltpu.VMEM((N, tokens, width), BF),
            pltpu.VMEM((N, tokens, width), BF),
            pltpu.VMEM((2, width, keys), F32),
            pltpu.VMEM((count, BLOCK), F32),
            pltpu.VMEM((count, 2 * BLOCK), BF),
            pltpu.VMEM((ROWS, NBB, count), BF),
            pltpu.VMEM((2, N, ROWS, share, BLOCK), BF),
            pltpu.VMEM((2 * N, ROWS, share, BLOCK), BF),
            pltpu.VMEM((N, ROWS, share, BLOCK), BF),
            pltpu.VMEM((ROWS, share, BLOCK), F32),
            pltpu.VMEM((width, keys), F32),
            pltpu.VMEM((2, width, BLOCK), F32),
            pltpu.VMEM((tokens, BLOCK), F32),
            pltpu.VMEM((count, BLOCK), F32),
            pltpu.VMEM((count, 2 * BLOCK), BF),
            pltpu.VMEM((2, ROWS, NBB, count), BF),
            pltpu.VMEM((2,) + bucket.shape, jnp.int32),
            pltpu.VMEM((2,) + bucket.shape, jnp.int32),
            pltpu.VMEM((1, model), F32),
            pltpu.VMEM(bucket.shape, jnp.int32),
            pltpu.VMEM(bucket.shape, jnp.int32),
            pltpu.VMEM(flat, F32),
            pltpu.VMEM(flat, F32),
            pltpu.VMEM(flat, F32),
            pltpu.VMEM(flat, F32),
            pltpu.VMEM((tokens, BLOCK), F32),
            pltpu.VMEM((ROWS, BLOCK, NBB), BF),
            dma((N,)), dma((N,)), dma((8,)), dma((8,)), dma((N,)), dma((N,)), dma((N,)), dma((N,)),
            dma((2 * N,)), dma((2 * N,)), dma((N,)), dma((N,)), dma((8,)), dma((8,)), dma((8,)), dma((8,)),
        ],
        compiler_params=pltpu.CompilerParams(
            collective_id=0, has_side_effects=True, vmem_limit_bytes=60 * 1024 * 1024),
        name="step",
    )(hidden_states, gain_row, key_weight, key_cotangent, bucket, sign_bits, momentum.reshape(flat), error.reshape(flat))
    grad, momentum_new, error_new, update = pl.pallas_call(
        results_kernel,
        out_shape=(
            jax.ShapeDtypeStruct((tokens, model), BF),
            jax.ShapeDtypeStruct(flat, F32),
            jax.ShapeDtypeStruct(flat, F32),
            jax.ShapeDtypeStruct((width, keys), F32),
        ),
        in_specs=[any_spec] * 7,
        out_specs=(any_spec,) * 4,
        scratch_shapes=[
            pltpu.VMEM((N, tokens, width), BF),
            pltpu.VMEM((tokens, model), BF),
            pltpu.VMEM((tokens, model), BF),
            pltpu.VMEM((1, model), F32),
            pltpu.VMEM((tokens, BLOCK), F32),
            pltpu.VMEM(flat, F32),
            pltpu.VMEM(flat, F32),
            pltpu.VMEM((width, keys), F32),
            dma((8,)), dma((8,)), dma((8,)), dma((5,)), dma((3,)),
        ],
        compiler_params=pltpu.CompilerParams(vmem_limit_bytes=60 * 1024 * 1024),
        name="tail",
    )(returned, hidden_states, gain_row, factor, momentum_new, error_new, update)
    return grad, momentum_new.reshape(momentum.shape), error_new.reshape(error.shape), update


def solution(mesh):
    in_specs = (
        P(("dp", "fsdp"), None),
        P(),
        P("fsdp", None),
        P(("dp", "fsdp"), None),
        P(None, "fsdp"),
        P(None, "fsdp"),
        P("fsdp", None, "dp"),
        P("fsdp", None, "dp"),
    )
    out_specs = (
        P(("dp", "fsdp"), None),
        P("fsdp", None, "dp"),
        P("fsdp", None, "dp"),
        P("fsdp", None),
    )
    return jax.shard_map(
        on_device, mesh=mesh, in_specs=in_specs, out_specs=out_specs, check_vma=False
    )
```
